32 devices in a mesh: grp: 4 (over x, core), dp: 4 (over z), seq: 2 (over y).
Axes of the slice: x: 2, y: 2, z: 4, core: 2. Of those that a mesh axis runs over, the one named last changes fastest.
Arguments:
- student_saved_input: bfloat16 [16, 256, 3584], P(('grp', 'dp'), 'seq'), may hold values from -6 to 6
- student_saved_query: bfloat16 [16, 256, 1792], P(('grp', 'dp'), 'seq'), may hold values from -600 to 600
- feature_cotangent: bfloat16 [16, 256, 1792], P(('grp', 'dp'), 'seq'), may hold values from -6 to 6
- feature_weights: bfloat16 [128, 896], replicated, may hold values from -0.5 to 0.5
- adapter_down_weight: bfloat16 [8, 3584], replicated, may hold values from -0.09375 to 0.09375
- adapter_up_weight: bfloat16 [8, 1792], replicated, may hold values from -0.09375 to 0.09375
- teacher_next_query: bfloat16 [16, 512, 1792], P(('grp', 'dp'), 'seq'), may hold values from -6 to 6
- teacher_next_key: bfloat16 [16, 512, 256], P(('grp', 'dp'), 'seq'), may hold values from -6 to 6
- teacher_next_value: bfloat16 [16, 512, 256], P(('grp', 'dp'), 'seq'), may hold values from -6 to 6
- positions: int32 [16, 512], P(('grp', 'dp'), 'seq'), may hold values from 0 to 511, each once within a row
Outputs:
- teacher_output: bfloat16 [16, 512, 1792], P(('grp', 'dp'), 'seq')
- grad_feature: float32 [128, 896], P('dp')
- grad_down: float32 [8, 3584], P(None, 'dp')
- up_gradient: float32 [8, 1792], P(None, 'dp')
The draws below stay inside these ranges and needn't reach their ends.
Inputs may be any that keep to these rules, and one draw needn't show every extreme that they name: `positions`: each sequence's row is a permutation of 0 to 511.
All inputs are finite; a program needn't handle non-finite values.
Results may differ from the reference program's by a relative error of at most 0.015.
Values may be sent and summed in bfloat16 or wider, within the bound.
A program may use at most 64 MiB of HBM per device.

```python
import jax
import jax.numpy as jnp
from jax import lax

MODEL_WIDTH = 3584
QUERY_HEADS = 14
KEY_VALUE_HEADS = 2
HEAD_SIZE = 128
F = 64
LOW_RANK = 8
TEACHER_BATCH = 16
SBATCH = 16
TEACHER_LENGTH = 512
SLEN = 256


def teacher_pair(key):
    group_width = QUERY_HEADS // KEY_VALUE_HEADS
    rows_of_queries = jnp.clip(jax.random.normal(jax.random.fold_in(key, 101), (TEACHER_BATCH, TEACHER_LENGTH, KEY_VALUE_HEADS, group_width, HEAD_SIZE), jnp.float32), -6.0, 6.0)
    rows_of_keys = jnp.clip(jax.random.normal(jax.random.fold_in(key, 102), (TEACHER_BATCH, TEACHER_LENGTH, KEY_VALUE_HEADS, HEAD_SIZE), jnp.float32), -6.0, 6.0)
    return (rows_of_queries.reshape(TEACHER_BATCH, TEACHER_LENGTH, QUERY_HEADS * HEAD_SIZE), rows_of_keys.reshape(TEACHER_BATCH, TEACHER_LENGTH, KEY_VALUE_HEADS * HEAD_SIZE))


def draw_teacher_next_query(key, part):
    return teacher_pair(key)[0].astype(jnp.bfloat16)


def draw_teacher_next_key(key, part):
    return teacher_pair(key)[1].astype(jnp.bfloat16)


def draw_student_saved_query(key, part):
    values = jnp.clip(jax.random.normal(jax.random.fold_in(key, 107), (SBATCH, SLEN, QUERY_HEADS * HEAD_SIZE), jnp.float32), -6.0, 6.0)
    return values.astype(jnp.bfloat16)


def block_scale(key, shape, shards, low, largest):
    factor_of, own = 1.0, jax.random.fold_in(key, 6)
    for position, parts in shards:
        draws = jnp.exp(jax.random.uniform(jax.random.fold_in(own, position), (parts,), jnp.float32, low / len(shards), largest / len(shards)))
        factor_of = factor_of * jnp.repeat(draws, shape[position] // parts).reshape([-1 if axis == position else 1 for axis in range(len(shape))])
    return factor_of


def bell_draw(own_key, extent, scale, most, shards=(), held_as=jnp.bfloat16):
    entries = jax.random.normal(own_key, extent, jnp.float32) * scale
    if len(shards) > 0:
        entries = block_scale(own_key, extent, shards, -0.22, 0.18) * entries
    return jnp.clip(entries, min=-most, max=most).astype(held_as)


def setup_inputs(seed: int = 0) -> dict:
    key_of = jax.random.split(jax.random.key(seed), 11)
    student_saved_input = bell_draw(key_of[0], (SBATCH, SLEN, MODEL_WIDTH), 1.0, 6.0, ((0, 16), (1, 2)))
    student_saved_query = draw_student_saved_query(jax.random.fold_in(key_of[10], 71), 0)
    feature_cotangent = bell_draw(key_of[2], (SBATCH, SLEN, QUERY_HEADS * 2 * F), 1.0, 6.0, ((0, 16), (1, 2)))
    feature_weights = bell_draw(key_of[3], (HEAD_SIZE, QUERY_HEADS * F), HEAD_SIZE ** -0.5, 0.5)
    adapter_down_weight = bell_draw(key_of[4], (LOW_RANK, MODEL_WIDTH), MODEL_WIDTH ** -0.5, 0.09375)
    adapter_up_weight = bell_draw(key_of[5], (LOW_RANK, QUERY_HEADS * HEAD_SIZE), MODEL_WIDTH ** -0.5, 0.09375)
    teacher_next_query = draw_teacher_next_query(jax.random.fold_in(key_of[10], 71), 0)
    teacher_next_key = draw_teacher_next_key(jax.random.fold_in(key_of[10], 71), 0)
    teacher_next_value = bell_draw(key_of[8], (TEACHER_BATCH, TEACHER_LENGTH, KEY_VALUE_HEADS * HEAD_SIZE), 1.0, 6.0, ((0, 16), (1, 2)))
    positions = jax.vmap(lambda own: jax.random.permutation(own, TEACHER_LENGTH))(jax.random.split(key_of[9], TEACHER_BATCH)).reshape((TEACHER_BATCH, TEACHER_LENGTH)).astype(jnp.int32)
    return {"student_saved_input": student_saved_input, "student_saved_query": student_saved_query, "feature_cotangent": feature_cotangent, "feature_weights": feature_weights, "adapter_down_weight": adapter_down_weight, "adapter_up_weight": adapter_up_weight, "teacher_next_query": teacher_next_query, "teacher_next_key": teacher_next_key, "teacher_next_value": teacher_next_value, "positions": positions}


adapter_scale = 2.0
masked_score = -1e30


def teacher_one(operands):
    rows_of_queries, rows_of_keys, rows_of_values, pos_rows = operands
    group_width = QUERY_HEADS // KEY_VALUE_HEADS
    heads_of_queries = rows_of_queries.astype(jnp.float32).reshape(TEACHER_LENGTH, KEY_VALUE_HEADS, group_width, HEAD_SIZE)
    heads_of_keys = rows_of_keys.astype(jnp.float32).reshape(TEACHER_LENGTH, KEY_VALUE_HEADS, HEAD_SIZE)
    heads_of_values = rows_of_values.astype(jnp.float32).reshape(TEACHER_LENGTH, KEY_VALUE_HEADS, HEAD_SIZE)
    score = jnp.einsum("qcgd,kcd->cgqk", heads_of_queries, heads_of_keys, precision=lax.Precision.HIGHEST) * (HEAD_SIZE ** -0.5)
    allowed = (pos_rows[None, :] <= pos_rows[:, None])[None, None]
    score = jnp.where(allowed, score, masked_score)
    row_max = jnp.max(score, axis=-1)
    weight = jnp.where(allowed, jnp.exp(score - row_max[..., None]), 0.0)
    denom = jnp.sum(weight, axis=-1)
    weight_b = lax.optimization_barrier(weight.astype(jnp.bfloat16)).astype(jnp.float32)
    mixed = jnp.einsum("cgqk,kcd->qcgd", weight_b, heads_of_values, precision=lax.Precision.HIGHEST)
    output = mixed / jnp.transpose(denom, (2, 0, 1))[..., None]
    return output.astype(jnp.bfloat16).reshape(TEACHER_LENGTH, QUERY_HEADS * HEAD_SIZE)


def reference(student_saved_input, student_saved_query, feature_cotangent, feature_weights, adapter_down_weight, adapter_up_weight, teacher_next_query, teacher_next_key, teacher_next_value, positions):
    teacher_output = lax.map(teacher_one, (teacher_next_query, teacher_next_key, teacher_next_value, positions))
    row_count = SBATCH * SLEN
    heads_of_queries = student_saved_query.astype(jnp.float32).reshape(row_count, QUERY_HEADS, HEAD_SIZE)
    map_heads = feature_weights.astype(jnp.float32).reshape(HEAD_SIZE, QUERY_HEADS, F)
    logits = jnp.einsum("shd,dhf->shf", heads_of_queries, map_heads, precision=lax.Precision.HIGHEST)
    prob_plus = jax.nn.softmax(logits, axis=-1)
    prob_minus = jax.nn.softmax(-logits, axis=-1)
    cotangent = feature_cotangent.astype(jnp.float32).reshape(row_count, QUERY_HEADS, 2 * F)
    cot_plus = cotangent[..., :F]
    cot_minus = cotangent[..., F:]
    dlogit = prob_plus * (cot_plus - jnp.sum(prob_plus * cot_plus, axis=-1, keepdims=True)) - prob_minus * (cot_minus - jnp.sum(prob_minus * cot_minus, axis=-1, keepdims=True))
    dlogit_b = lax.optimization_barrier(dlogit.astype(jnp.bfloat16)).astype(jnp.float32)
    grad_feature = jnp.einsum("shd,shf->dhf", heads_of_queries, dlogit_b, precision=lax.Precision.HIGHEST).reshape(HEAD_SIZE, QUERY_HEADS * F)
    query_gradient = jnp.einsum("shf,dhf->shd", dlogit_b, map_heads, precision=lax.Precision.HIGHEST).reshape(row_count, QUERY_HEADS * HEAD_SIZE).astype(jnp.bfloat16)
    input_rows = student_saved_input.reshape(row_count, MODEL_WIDTH)
    down_activation = jnp.dot(input_rows, adapter_down_weight.T, preferred_element_type=jnp.float32).astype(jnp.bfloat16)
    up_gradient = adapter_scale * jnp.dot(down_activation.T, query_gradient, preferred_element_type=jnp.float32)
    lowrank_gradient = (adapter_scale * jnp.dot(query_gradient, adapter_up_weight.T, preferred_element_type=jnp.float32)).astype(jnp.bfloat16)
    grad_down = jnp.dot(lowrank_gradient.T, input_rows, preferred_element_type=jnp.float32)
    return (teacher_output, grad_feature, grad_down, up_gradient)
```

```python
import functools

import jax
import jax.numpy as jnp
from jax import lax
from jax.experimental import pallas as pl
from jax.experimental.pallas import tpu as pltpu
from jax.sharding import PartitionSpec as P

MESH = pl.DeviceIdType.MESH
HEAD_SIZE = 128
F = 64
LANES = 128
ROWS = 8
ADAPTER_SCALE = 2.0
MASKED = -1e30
LOG2E = 1.4426950408889634
BF16 = jnp.bfloat16
F32 = jnp.float32


def dot(a, b, dims=((1,), (0,))):
    return lax.dot_general(a, b, (dims, ((), ())), preferred_element_type=F32)


class Plan:
    def __init__(self, n_grp, n_dp, n_seq, feature_shape, down_width, up_width):
        self.n_grp, self.n_dp, self.n_seq = n_grp, n_dp, n_seq
        self.plane = n_grp // 2 * n_seq
        self.feature_rows = feature_shape[0] // n_dp
        self.down_width, self.up_width = down_width // n_dp, up_width // n_dp
        halves = []
        pairs = max(1, self.feature_rows // 16)
        for block in range(pairs):
            for tile in range(feature_shape[1] // LANES):
                for row in range(block * 16, min(block * 16 + 16, self.feature_rows), ROWS):
                    halves.append((0, row, tile * LANES, LANES))
        for which, width in ((1, self.down_width), (2, self.up_width)):
            for begin in range(0, width, LANES):
                halves.append((which, 0, begin, min(LANES, width - begin)))
        self.halves = halves
        self.used = (len(halves) + 1) // 2
        step = 2 * self.plane
        self.per = -(-self.used // step)
        self.units = self.per * step

    def where(self, unit):
        core, rest = divmod(unit, self.plane * self.per)
        return (core,) + divmod(rest, self.per)


def kernel(
    plan,
    x_hbm, sq_hbm, cot_hbm, w_hbm, ad_hbm, au_hbm, tq_hbm, tk_hbm, tv_hbm, pos_hbm,
    out_ref, gf_out, gd_out, gu_out,
    x_ref, sq_ref, cot_ref, w_ref, ad_ref, au_ref, tq_ref, k_ref, v_ref, pos_ref,
    bias_ref, dq_ref, gf_ref, gd_ref, gu_ref,
    g_ref, r1_ref, s1_ref, r2_ref, s2_ref, r3_ref, a_ref,
    load_sem, kv_send, kv_recv, core_send, core_recv, plane_send, plane_recv,
    dp_send, dp_recv, all_send, all_recv,
):
    n_dp, n_seq, n_grp, n_plane, per = plan.n_dp, plan.n_seq, plan.n_grp, plan.plane, plan.per
    grp, dp, seq = lax.axis_index("grp"), lax.axis_index("dp"), lax.axis_index("seq")
    core = lax.rem(grp, 2)
    mine = lax.div(grp, 2) * n_seq + seq

    def in_plane(index, which_core):
        return {"grp": lax.div(index, n_seq) * 2 + which_core, "dp": dp, "seq": lax.rem(index, n_seq)}

    loads = []
    for n, (src, dst) in enumerate(
        (
            (pos_hbm, pos_ref.at[0]), (tk_hbm.at[0], k_ref.at[0]), (tv_hbm.at[0], v_ref.at[0]),
            (w_hbm, w_ref), (sq_hbm.at[0], sq_ref), (cot_hbm.at[0], cot_ref), (ad_hbm, ad_ref),
            (x_hbm.at[0], x_ref), (au_hbm, au_ref), (tq_hbm.at[0], tq_ref),
        )
    ):
        copy = pltpu.make_async_copy(src, dst, load_sem.at[n])
        copy.start()
        loads.append(copy)

    barrier = pltpu.get_barrier_semaphore()
    greeted = 0
    for j in range(1, n_plane):
        for other in range(2):
            pl.semaphore_signal(
                barrier, inc=1, device_id=in_plane(lax.rem(mine + j, n_plane), other), device_id_type=MESH
            )
            greeted += 1
    partner = {"grp": grp + 1 - 2 * core, "dp": dp, "seq": seq}
    pl.semaphore_signal(barrier, inc=1, device_id=partner, device_id_type=MESH)
    for j in range(1, n_dp):
        pl.semaphore_signal(
            barrier, inc=1, device_id={"grp": grp, "dp": lax.rem(dp + j, n_dp), "seq": seq}, device_id_type=MESH
        )
    greeted += n_dp

    for unit in range(plan.used, plan.units):
        c, p, k = plan.where(unit)
        g_ref[c, p, :, k] = jnp.zeros((n_dp, 16, LANES), BF16)

    for n in range(3):
        loads[n].wait()
    pl.semaphore_wait(barrier, greeted)

    kv_copies = []
    for n, ref in enumerate((pos_ref, k_ref, v_ref)):
        for j in range(1, n_seq):
            copy = pltpu.make_async_remote_copy(
                src_ref=ref.at[0], dst_ref=ref.at[j],
                send_sem=kv_send.at[n, j], recv_sem=kv_recv.at[n, j],
                device_id={"grp": grp, "dp": dp, "seq": lax.rem(seq + j, n_seq)}, device_id_type=MESH,
            )
            copy.start()
            kv_copies.append(copy)

    rows = sq_ref.shape[0]
    lane = lax.broadcasted_iota(jnp.int32, (rows, LANES), 1)
    first = lane < F
    wide = lax.broadcasted_iota(jnp.int32, (2 * LANES, LANES), 1) < F
    depth = lax.broadcasted_iota(jnp.int32, (2 * LANES, LANES), 0)
    ones = ((lax.rem(depth, LANES) < F) == wide).astype(F32).astype(BF16)
    w_half = lax.broadcasted_iota(jnp.int32, (HEAD_SIZE, LANES), 1) < F

    def half_max(values):
        one = jnp.max(jnp.where(first, values, -jnp.inf), axis=1, keepdims=True)
        two = jnp.max(jnp.where(first, -jnp.inf, values), axis=1, keepdims=True)
        return jnp.where(first, one, two)

    def half_sum(values):
        stack = jnp.concatenate(values, axis=0)
        high = stack.astype(BF16)
        low = (stack - high.astype(F32)).astype(BF16)
        sums = dot(jnp.concatenate([high, low], axis=1), ones)
        return [sums[n * rows:(n + 1) * rows] for n in range(len(values))]

    for n in range(3, 6):
        loads[n].wait()
    for j in range(w_ref.shape[1] // LANES):
        q2 = sq_ref[:, 2 * LANES * j:2 * LANES * (j + 1)]
        w = w_ref[:, LANES * j:LANES * (j + 1)].astype(F32)
        w2 = jnp.concatenate([jnp.where(w_half, w, 0.0), jnp.where(w_half, 0.0, w)], axis=0).astype(BF16)
        logit = dot(q2, w2)
        plus = jnp.exp(logit - half_max(logit))
        minus = jnp.exp(-logit - half_max(-logit))
        cot_a = cot_ref[:, 2 * LANES * j:2 * LANES * j + LANES].astype(F32)
        cot_b = cot_ref[:, 2 * LANES * j + LANES:2 * LANES * (j + 1)].astype(F32)
        cot_plus = jnp.where(first, cot_a, pltpu.roll(cot_b, F, 1))
        cot_minus = jnp.where(first, pltpu.roll(cot_a, F, 1), cot_b)
        sum_p, sum_m, sum_pc, sum_mc = half_sum([plus, minus, plus * cot_plus, minus * cot_minus])
        inv_p, inv_m = 1.0 / sum_p, 1.0 / sum_m
        dlogit = plus * inv_p * (cot_plus - sum_pc * inv_p) - minus * inv_m * (cot_minus - sum_mc * inv_m)
        dlogit_b = dlogit.astype(BF16)
        grad = dot(q2, dlogit_b, ((0,), (0,)))
        gf_ref[:, LANES * j:LANES * (j + 1)] = jnp.where(w_half, grad[:HEAD_SIZE], grad[HEAD_SIZE:])
        dq_ref[:, 2 * LANES * j:2 * LANES * (j + 1)] = dot(dlogit_b, w2, ((1,), (1,))).astype(BF16)
    for n in range(6, 9):
        loads[n].wait()
    down_act = dot(ad_ref[...], x_ref[...], ((1,), (1,))).astype(BF16)
    gu_ref[...] = ADAPTER_SCALE * dot(down_act, dq_ref[...])
    dlow = (ADAPTER_SCALE * dot(au_ref[...], dq_ref[...], ((1,), (1,)))).astype(BF16)
    gd_ref[...] = dot(dlow, x_ref[...])

    def half_unit(index, d):
        if index >= len(plan.halves):
            return jnp.zeros((ROWS, LANES), F32)
        which, row, begin, width = plan.halves[index]
        if which == 0:
            row = d * plan.feature_rows + row
            return gf_ref[row:row + ROWS, begin:begin + LANES]
        ref, own = ((gd_ref, plan.down_width), (gu_ref, plan.up_width))[which - 1]
        begin = d * own + begin
        value = ref[:, begin:begin + width]
        if width < LANES:
            value = jnp.concatenate([value, jnp.zeros((ROWS, LANES - width), F32)], axis=1)
        return value

    for unit in range(plan.used):
        c, p, k = plan.where(unit)
        for d in range(n_dp):
            g_ref[c, p, d, k] = jnp.concatenate(
                [half_unit(2 * unit, d), half_unit(2 * unit + 1, d)], axis=0
            ).astype(BF16)

    core_copy = pltpu.make_async_remote_copy(
        src_ref=g_ref.at[1 - core], dst_ref=r1_ref, send_sem=core_send, recv_sem=core_recv,
        device_id=partner, device_id_type=MESH,
    )
    core_copy.start()
    pending = []

    def plane_stage():
        core_copy.wait_recv()
        s1_ref[...] = (g_ref[core].astype(F32) + r1_ref[...].astype(F32)).astype(BF16)
        for j in range(1, n_plane):
            other = lax.rem(mine + j, n_plane)
            copy = pltpu.make_async_remote_copy(
                src_ref=s1_ref.at[other], dst_ref=r2_ref.at[j],
                send_sem=plane_send.at[j], recv_sem=plane_recv.at[j],
                device_id=in_plane(other, core), device_id_type=MESH,
            )
            copy.start()
            pending.append(copy)

    def dp_stage():
        total = s1_ref[mine].astype(F32)
        for j in range(1, n_plane):
            pending[j - 1].wait_recv()
            total = total + r2_ref[j].astype(F32)
        s2_ref[...] = total.astype(BF16)
        for j in range(1, n_dp):
            other = lax.rem(dp + j, n_dp)
            copy = pltpu.make_async_remote_copy(
                src_ref=s2_ref.at[other], dst_ref=r3_ref.at[j],
                send_sem=dp_send.at[j], recv_sem=dp_recv.at[j],
                device_id={"grp": grp, "dp": other, "seq": seq}, device_id_type=MESH,
            )
            copy.start()
            pending.append(copy)

    def gather_stage():
        total = s2_ref[dp].astype(F32)
        for j in range(1, n_dp):
            pending[n_plane - 1 + j - 1].wait_recv()
            total = total + r3_ref[j].astype(F32)
        a_ref[core, mine] = total.astype(BF16)
        for j in range(n_plane):
            for flip in range(2):
                if j == 0 and flip == 0:
                    continue
                copy = pltpu.make_async_remote_copy(
                    src_ref=a_ref.at[core, mine], dst_ref=a_ref.at[core, mine],
                    send_sem=all_send.at[2 * j + flip], recv_sem=all_recv.at[2 * j + flip],
                    device_id=in_plane(lax.rem(mine + j, n_plane), core + flip * (1 - 2 * core)),
                    device_id_type=MESH,
                )
                copy.start()
                pending.append(copy)

    for copy in kv_copies:
        copy.wait_recv()
    loads[9].wait()
    queries = tq_ref.shape[0]
    keys = k_ref.shape[1]
    own_pos = pos_ref[0].astype(F32)
    for begin in range(0, queries, LANES):
        column = jnp.transpose(jnp.broadcast_to(own_pos[:, begin:begin + LANES], (LANES, LANES)))
        for j in range(n_seq):
            key_pos = pos_ref[j].astype(F32)
            for at in range(0, keys, LANES):
                bias_ref[begin:begin + LANES, j * keys + at:j * keys + at + LANES] = jnp.where(
                    key_pos[:, at:at + LANES] <= column, 0.0, MASKED
                )
    heads = tq_ref.shape[1] // HEAD_SIZE
    group = heads // (k_ref.shape[2] // HEAD_SIZE)
    factor = HEAD_SIZE ** (-0.5) * LOG2E
    stages = {1 * heads // 14: plane_stage, 7 * heads // 14: dp_stage, 12 * heads // 14: gather_stage}
    ones_v = jnp.ones((n_seq * keys, HEAD_SIZE), BF16)
    for h in range(heads):
        if h in stages:
            stages[h]()
        at = h // group * HEAD_SIZE
        k_all = k_ref[:, :, at:at + HEAD_SIZE].reshape(n_seq * keys, HEAD_SIZE)
        v_all = jnp.concatenate(
            [v_ref[:, :, at:at + HEAD_SIZE].reshape(n_seq * keys, HEAD_SIZE), ones_v], axis=1
        )
        score = dot(tq_ref[:, h * HEAD_SIZE:(h + 1) * HEAD_SIZE], k_all, ((1,), (1,))) + bias_ref[...]
        top = jnp.max(score, axis=1, keepdims=True)
        weight = jnp.exp2((score - top) * factor).astype(BF16)
        mixed = dot(weight, v_all)
        out_ref[0, :, h * HEAD_SIZE:(h + 1) * HEAD_SIZE] = (
            mixed[:, :HEAD_SIZE] / mixed[:, HEAD_SIZE:]
        ).astype(BF16)

    for copy in pending[n_plane - 1 + n_dp - 1:]:
        copy.wait_recv()
    for index, (which, row, begin, width) in enumerate(plan.halves):
        c, p, k = plan.where(index // 2)
        half = index % 2 * ROWS
        value = a_ref[c, p, k].astype(F32)[half:half + ROWS, :width]
        (gf_out, gd_out, gu_out)[which][row:row + ROWS, begin:begin + width] = value
    core_copy.wait_send()
    for copy in kv_copies + pending:
        copy.wait_send()


def on_device(mesh_shape, *args):
    x, sq, cot, w, ad, au, tq, tk, tv, pos = args
    n_grp, n_dp, n_seq = mesh_shape["grp"], mesh_shape["dp"], mesh_shape["seq"]
    plan = Plan(n_grp, n_dp, n_seq, w.shape, x.shape[2], sq.shape[2])
    n_plane, per = plan.plane, plan.per
    rows, queries, keys = sq.shape[1], tq.shape[1], tk.shape[1]
    vm, dma = pltpu.VMEM, pltpu.SemaphoreType.DMA
    unit = (16, LANES)
    return pl.pallas_call(
        functools.partial(kernel, plan),
        out_shape=(
            jax.ShapeDtypeStruct(tq.shape, BF16),
            jax.ShapeDtypeStruct((plan.feature_rows, w.shape[1]), F32),
            jax.ShapeDtypeStruct((ad.shape[0], plan.down_width), F32),
            jax.ShapeDtypeStruct((au.shape[0], plan.up_width), F32),
        ),
        in_specs=[pl.BlockSpec(memory_space=pl.ANY)] * 10,
        out_specs=[pl.BlockSpec(memory_space=pltpu.VMEM)] * 4,
        scratch_shapes=[
            vm(x.shape[1:], BF16), vm(sq.shape[1:], BF16), vm(cot.shape[1:], BF16), vm(w.shape, BF16),
            vm(ad.shape, BF16), vm(au.shape, BF16), vm(tq.shape[1:], BF16),
            vm((n_seq, keys, tk.shape[2]), BF16), vm((n_seq, keys, tv.shape[2]), BF16),
            vm((n_seq, 1, keys), jnp.int32),
            vm((queries, n_seq * keys), F32), vm((rows, sq.shape[2]), BF16),
            vm(w.shape, F32), vm(ad.shape, F32), vm(au.shape, F32),
            vm((2, n_plane, n_dp, per) + unit, BF16),
            vm((n_plane, n_dp, per) + unit, BF16), vm((n_plane, n_dp, per) + unit, BF16),
            vm((n_plane, n_dp, per) + unit, BF16),
            vm((n_dp, per) + unit, BF16), vm((n_dp, per) + unit, BF16),
            vm((2, n_plane, per) + unit, BF16),
            dma((10,)), dma((3, n_seq)), dma((3, n_seq)), dma, dma,
            dma((n_plane,)), dma((n_plane,)), dma((n_dp,)), dma((n_dp,)),
            dma((2 * n_plane,)), dma((2 * n_plane,)),
        ],
        compiler_params=pltpu.CompilerParams(
            collective_id=0, has_side_effects=True, vmem_limit_bytes=48 * 2**20
        ),
    )(*args)


def solution(mesh):
    rows = P(("grp", "dp"), "seq", None)
    return jax.shard_map(
        functools.partial(on_device, dict(mesh.shape)),
        mesh=mesh,
        in_specs=(rows, rows, rows, P(), P(), P(), rows, rows, rows, P(("grp", "dp"), "seq")),
        out_specs=(rows, P("dp", None), P(None, "dp"), P(None, "dp")),
        check_vma=False,
    )
```

```python
import functools

import jax
import jax.numpy as jnp
from jax import lax
from jax.experimental import pallas as pl
from jax.experimental.pallas import tpu as pltpu
from jax.sharding import PartitionSpec as P

MESH = pl.DeviceIdType.MESH
HEAD_SIZE = 128
F = 64
LANES = 128
ROWS = 8
ADAPTER_SCALE = 2.0
MASKED = -1e30
VMEM_BYTES = 67043328
PIECES = 4
LOG2E = 1.4426950408889634
BF16 = jnp.bfloat16
F32 = jnp.float32


def dot(a, b, dims=((1,), (0,))):
    return lax.dot_general(a, b, (dims, ((), ())), preferred_element_type=F32)


class Plan:
    def __init__(self, n_grp, n_dp, n_seq, feature_shape, down_width, up_width):
        self.n_grp, self.n_dp, self.n_seq = n_grp, n_dp, n_seq
        self.plane = n_grp // 2 * n_seq
        self.feature_rows = feature_shape[0] // n_dp
        self.down_width, self.up_width = down_width // n_dp, up_width // n_dp
        halves = []
        pairs = max(1, self.feature_rows // 16)
        for block in range(pairs):
            for tile in range(feature_shape[1] // LANES):
                for row in range(block * 16, min(block * 16 + 16, self.feature_rows), ROWS):
                    halves.append((0, row, tile * LANES, LANES))
        for which, width in ((1, self.down_width), (2, self.up_width)):
            for begin in range(0, width, LANES):
                halves.append((which, 0, begin, min(LANES, width - begin)))
        self.halves = halves
        self.used = (len(halves) + 1) // 2
        step = 2 * self.plane
        self.per = -(-self.used // step)
        self.units = self.per * step

    def where(self, unit):
        core, rest = divmod(unit, self.plane * self.per)
        return (core,) + divmod(rest, self.per)


def kernel(
    plan,
    x_hbm, sq_hbm, cot_hbm, w_hbm, ad_hbm, au_hbm, tq_hbm, tk_hbm, tv_hbm, pos_hbm,
    out_hbm, gf_out, gd_out, gu_out,
    x_ref, sq_ref, cot_ref, w_ref, ad_ref, au_ref, tq_ref, k_ref, v_ref, pos_ref,
    bias_ref, dq_ref, gf_ref, gd_ref, gu_ref,
    g_ref, r1_ref, s1_ref, r2_ref, s2_ref, r3_ref, a_ref,
    load_sem, kv_send, kv_recv, core_send, core_recv, plane_send, plane_recv,
    dp_send, dp_recv, all_send, all_recv, out_ref, out_sem,
):
    n_dp, n_seq, n_grp, n_plane, per = plan.n_dp, plan.n_seq, plan.n_grp, plan.plane, plan.per
    grp, dp, seq = lax.axis_index("grp"), lax.axis_index("dp"), lax.axis_index("seq")
    core = lax.rem(grp, 2)
    mine = lax.div(grp, 2) * n_seq + seq

    def in_plane(index, which_core):
        return {"grp": lax.div(index, n_seq) * 2 + which_core, "dp": dp, "seq": lax.rem(index, n_seq)}

    loads = []
    for n, (src, dst) in enumerate(
        (
            (pos_hbm, pos_ref.at[0]), (tk_hbm.at[0], k_ref.at[0]), (tv_hbm.at[0], v_ref.at[0]),
            (w_hbm, w_ref), (sq_hbm.at[0], sq_ref), (cot_hbm.at[0], cot_ref), (ad_hbm, ad_ref),
            (x_hbm.at[0], x_ref), (au_hbm, au_ref), (tq_hbm.at[0], tq_ref),
        )
    ):
        copy = pltpu.make_async_copy(src, dst, load_sem.at[n])
        copy.start()
        loads.append(copy)

    barrier = pltpu.get_barrier_semaphore()
    greeted = 0
    for j in range(1, n_plane):
        for other in range(2):
            pl.semaphore_signal(
                barrier, inc=1, device_id=in_plane(lax.rem(mine + j, n_plane), other), device_id_type=MESH
            )
            greeted += 1
    partner = {"grp": grp + 1 - 2 * core, "dp": dp, "seq": seq}
    pl.semaphore_signal(barrier, inc=1, device_id=partner, device_id_type=MESH)
    for j in range(1, n_dp):
        pl.semaphore_signal(
            barrier, inc=1, device_id={"grp": grp, "dp": lax.rem(dp + j, n_dp), "seq": seq}, device_id_type=MESH
        )
    greeted += n_dp

    for unit in range(plan.used, plan.units):
        c, p, k = plan.where(unit)
        g_ref[c, p, :, k] = jnp.zeros((n_dp, 16, LANES), BF16)

    for n in range(3):
        loads[n].wait()
    pl.semaphore_wait(barrier, greeted)

    kv_copies = []
    for n, ref in enumerate((pos_ref, k_ref, v_ref)):
        for j in range(1, n_seq):
            copy = pltpu.make_async_remote_copy(
                src_ref=ref.at[0], dst_ref=ref.at[j],
                send_sem=kv_send.at[n, j], recv_sem=kv_recv.at[n, j],
                device_id={"grp": grp, "dp": dp, "seq": lax.rem(seq + j, n_seq)}, device_id_type=MESH,
            )
            copy.start()
            kv_copies.append(copy)

    rows = sq_ref.shape[0]
    lane = lax.broadcasted_iota(jnp.int32, (rows, LANES), 1)
    first = lane < F
    wide = lax.broadcasted_iota(jnp.int32, (2 * LANES, LANES), 1) < F
    depth = lax.broadcasted_iota(jnp.int32, (2 * LANES, LANES), 0)
    ones = ((lax.rem(depth, LANES) < F) == wide).astype(F32).astype(BF16)
    w_half = lax.broadcasted_iota(jnp.int32, (HEAD_SIZE, LANES), 1) < F

    def half_max(values):
        one = jnp.max(jnp.where(first, values, -jnp.inf), axis=1, keepdims=True)
        two = jnp.max(jnp.where(first, -jnp.inf, values), axis=1, keepdims=True)
        return jnp.where(first, one, two)

    def half_sum(values):
        stack = jnp.concatenate(values, axis=0)
        high = stack.astype(BF16)
        low = (stack - high.astype(F32)).astype(BF16)
        sums = dot(jnp.concatenate([high, low], axis=1), ones)
        return [sums[n * rows:(n + 1) * rows] for n in range(len(values))]

    for n in range(3, 6):
        loads[n].wait()
    for j in range(w_ref.shape[1] // LANES):
        q2 = sq_ref[:, 2 * LANES * j:2 * LANES * (j + 1)]
        w = w_ref[:, LANES * j:LANES * (j + 1)].astype(F32)
        w2 = jnp.concatenate([jnp.where(w_half, w, 0.0), jnp.where(w_half, 0.0, w)], axis=0).astype(BF16)
        logit = dot(q2, w2)
        plus = jnp.exp(logit - half_max(logit))
        minus = jnp.exp(-logit - half_max(-logit))
        cot_a = cot_ref[:, 2 * LANES * j:2 * LANES * j + LANES].astype(F32)
        cot_b = cot_ref[:, 2 * LANES * j + LANES:2 * LANES * (j + 1)].astype(F32)
        cot_plus = jnp.where(first, cot_a, pltpu.roll(cot_b, F, 1))
        cot_minus = jnp.where(first, pltpu.roll(cot_a, F, 1), cot_b)
        sum_p, sum_m, sum_pc, sum_mc = half_sum([plus, minus, plus * cot_plus, minus * cot_minus])
        inv_p, inv_m = 1.0 / sum_p, 1.0 / sum_m
        dlogit = plus * inv_p * (cot_plus - sum_pc * inv_p) - minus * inv_m * (cot_minus - sum_mc * inv_m)
        dlogit_b = dlogit.astype(BF16)
        grad = dot(q2, dlogit_b, ((0,), (0,)))
        gf_ref[:, LANES * j:LANES * (j + 1)] = jnp.where(w_half, grad[:HEAD_SIZE], grad[HEAD_SIZE:])
        dq_ref[:, 2 * LANES * j:2 * LANES * (j + 1)] = dot(dlogit_b, w2, ((1,), (1,))).astype(BF16)
    for n in range(6, 9):
        loads[n].wait()
    down_act = dot(ad_ref[...], x_ref[...], ((1,), (1,))).astype(BF16)
    gu_ref[...] = ADAPTER_SCALE * dot(down_act, dq_ref[...])
    dlow = (ADAPTER_SCALE * dot(au_ref[...], dq_ref[...], ((1,), (1,)))).astype(BF16)
    gd_ref[...] = dot(dlow, x_ref[...])

    def half_unit(index, d):
        if index >= len(plan.halves):
            return jnp.zeros((ROWS, LANES), F32)
        which, row, begin, width = plan.halves[index]
        if which == 0:
            row = d * plan.feature_rows + row
            return gf_ref[row:row + ROWS, begin:begin + LANES]
        ref, own = ((gd_ref, plan.down_width), (gu_ref, plan.up_width))[which - 1]
        begin = d * own + begin
        value = ref[:, begin:begin + width]
        if width < LANES:
            value = jnp.concatenate([value, jnp.zeros((ROWS, LANES - width), F32)], axis=1)
        return value

    for unit in range(plan.used):
        c, p, k = plan.where(unit)
        for d in range(n_dp):
            g_ref[c, p, d, k] = jnp.concatenate(
                [half_unit(2 * unit, d), half_unit(2 * unit + 1, d)], axis=0
            ).astype(BF16)

    core_copy = pltpu.make_async_remote_copy(
        src_ref=g_ref.at[1 - core], dst_ref=r1_ref, send_sem=core_send, recv_sem=core_recv,
        device_id=partner, device_id_type=MESH,
    )
    core_copy.start()
    pending = []

    def plane_stage():
        core_copy.wait_recv()
        s1_ref[...] = (g_ref[core].astype(F32) + r1_ref[...].astype(F32)).astype(BF16)
        for j in range(1, n_plane):
            other = lax.rem(mine + j, n_plane)
            copy = pltpu.make_async_remote_copy(
                src_ref=s1_ref.at[other], dst_ref=r2_ref.at[j],
                send_sem=plane_send.at[j], recv_sem=plane_recv.at[j],
                device_id=in_plane(other, core), device_id_type=MESH,
            )
            copy.start()
            pending.append(copy)

    def dp_stage():
        total = s1_ref[mine].astype(F32)
        for j in range(1, n_plane):
            pending[j - 1].wait_recv()
            total = total + r2_ref[j].astype(F32)
        s2_ref[...] = total.astype(BF16)
        for j in range(1, n_dp):
            other = lax.rem(dp + j, n_dp)
            copy = pltpu.make_async_remote_copy(
                src_ref=s2_ref.at[other], dst_ref=r3_ref.at[j],
                send_sem=dp_send.at[j], recv_sem=dp_recv.at[j],
                device_id={"grp": grp, "dp": other, "seq": seq}, device_id_type=MESH,
            )
            copy.start()
            pending.append(copy)

    def gather_stage():
        total = s2_ref[dp].astype(F32)
        for j in range(1, n_dp):
            pending[n_plane - 1 + j - 1].wait_recv()
            total = total + r3_ref[j].astype(F32)
        a_ref[core, mine] = total.astype(BF16)
        for j in range(n_plane):
            for flip in range(2):
                if j == 0 and flip == 0:
                    continue
                copy = pltpu.make_async_remote_copy(
                    src_ref=a_ref.at[core, mine], dst_ref=a_ref.at[core, mine],
                    send_sem=all_send.at[2 * j + flip], recv_sem=all_recv.at[2 * j + flip],
                    device_id=in_plane(lax.rem(mine + j, n_plane), core + flip * (1 - 2 * core)),
                    device_id_type=MESH,
                )
                copy.start()
                pending.append(copy)

    for copy in kv_copies:
        copy.wait_recv()
    loads[9].wait()
    queries = tq_ref.shape[0]
    keys = k_ref.shape[1]
    own_pos = pos_ref[0].astype(F32)
    for begin in range(0, queries, LANES):
        column = jnp.transpose(jnp.broadcast_to(own_pos[:, begin:begin + LANES], (LANES, LANES)))
        for j in range(n_seq):
            key_pos = pos_ref[j].astype(F32)
            for at in range(0, keys, LANES):
                bias_ref[begin:begin + LANES, j * keys + at:j * keys + at + LANES] = jnp.where(
                    key_pos[:, at:at + LANES] <= column, 0.0, MASKED
                )
    heads = tq_ref.shape[1] // HEAD_SIZE
    group = heads // (k_ref.shape[2] // HEAD_SIZE)
    factor = HEAD_SIZE ** (-0.5) * LOG2E
    stages = {1 * heads // 14: plane_stage, 7 * heads // 14: dp_stage, 12 * heads // 14: gather_stage}
    ones_v = jnp.ones((n_seq * keys, HEAD_SIZE), BF16)
    outs = []
    for h in range(heads):
        if h in stages:
            stages[h]()
        at = h // group * HEAD_SIZE
        k_all = k_ref[:, :, at:at + HEAD_SIZE].reshape(n_seq * keys, HEAD_SIZE)
        v_all = jnp.concatenate(
            [v_ref[:, :, at:at + HEAD_SIZE].reshape(n_seq * keys, HEAD_SIZE), ones_v], axis=1
        )
        score = dot(tq_ref[:, h * HEAD_SIZE:(h + 1) * HEAD_SIZE], k_all, ((1,), (1,))) + bias_ref[...]
        top = jnp.max(score, axis=1, keepdims=True)
        weight = jnp.exp2((score - top) * factor).astype(BF16)
        mixed = dot(weight, v_all)
        own = pl.ds(h * HEAD_SIZE, HEAD_SIZE)
        out_ref[:, own] = (mixed[:, :HEAD_SIZE] / mixed[:, HEAD_SIZE:]).astype(BF16)
        if h:
            outs[-1].start()
        outs.append(pltpu.make_async_copy(out_ref.at[:, own], out_hbm.at[0, :, own], out_sem.at[h]))
    outs[-1].start()

    for copy in pending[n_plane - 1 + n_dp - 1:]:
        copy.wait_recv()
    for index, (which, row, begin, width) in enumerate(plan.halves):
        c, p, k = plan.where(index // 2)
        half = index % 2 * ROWS
        value = a_ref[c, p, k].astype(F32)[half:half + ROWS, :width]
        (gf_out, gd_out, gu_out)[which][row:row + ROWS, begin:begin + width] = value
    for copy in outs:
        copy.wait()
    core_copy.wait_send()
    for copy in kv_copies + pending:
        copy.wait_send()


def write_out(*refs):
    sources, targets, held, load_sem, store_sem = refs[:4], refs[4:8], refs[8:12], refs[12], refs[13]
    rows = sources[0].shape[1] // PIECES
    parts = [(n, slice(None)) for n in range(1, 4)]
    parts += [(0, (0, pl.ds(piece * rows, rows))) for piece in range(PIECES)]
    loads = [
        pltpu.make_async_copy(sources[n].at[at], held[n].at[at], load_sem.at[i])
        for i, (n, at) in enumerate(parts)
    ]
    stores = [
        pltpu.make_async_copy(held[n].at[at], targets[n].at[at], store_sem.at[i])
        for i, (n, at) in enumerate(parts)
    ]
    for load in loads:
        load.start()
    for load, store in zip(loads, stores):
        load.wait()
        store.start()
    for store in stores:
        store.wait()


def on_device(mesh_shape, *args):
    x, sq, cot, w, ad, au, tq, tk, tv, pos = args
    n_grp, n_dp, n_seq = mesh_shape["grp"], mesh_shape["dp"], mesh_shape["seq"]
    plan = Plan(n_grp, n_dp, n_seq, w.shape, x.shape[2], sq.shape[2])
    n_plane, per = plan.plane, plan.per
    rows, queries, keys = sq.shape[1], tq.shape[1], tk.shape[1]
    vm, dma = pltpu.VMEM, pltpu.SemaphoreType.DMA
    unit = (16, LANES)
    shapes = (
        jax.ShapeDtypeStruct(tq.shape, BF16),
        jax.ShapeDtypeStruct((plan.feature_rows, w.shape[1]), F32),
        jax.ShapeDtypeStruct((ad.shape[0], plan.down_width), F32),
        jax.ShapeDtypeStruct((au.shape[0], plan.up_width), F32),
    )
    results = pl.pallas_call(
        functools.partial(kernel, plan),
        out_shape=shapes,
        in_specs=[pl.BlockSpec(memory_space=pl.ANY)] * 10,
        out_specs=[pl.BlockSpec(memory_space=pl.ANY)] + [pl.BlockSpec(memory_space=pltpu.VMEM)] * 3,
        scratch_shapes=[
            vm(x.shape[1:], BF16), vm(sq.shape[1:], BF16), vm(cot.shape[1:], BF16), vm(w.shape, BF16),
            vm(ad.shape, BF16), vm(au.shape, BF16), vm(tq.shape[1:], BF16),
            vm((n_seq, keys, tk.shape[2]), BF16), vm((n_seq, keys, tv.shape[2]), BF16),
            vm((n_seq, 1, keys), jnp.int32),
            vm((queries, n_seq * keys), F32), vm((rows, sq.shape[2]), BF16),
            vm(w.shape, F32), vm(ad.shape, F32), vm(au.shape, F32),
            vm((2, n_plane, n_dp, per) + unit, BF16),
            vm((n_plane, n_dp, per) + unit, BF16), vm((n_plane, n_dp, per) + unit, BF16),
            vm((n_plane, n_dp, per) + unit, BF16),
            vm((n_dp, per) + unit, BF16), vm((n_dp, per) + unit, BF16),
            vm((2, n_plane, per) + unit, BF16),
            dma((10,)), dma((3, n_seq)), dma((3, n_seq)), dma, dma,
            dma((n_plane,)), dma((n_plane,)), dma((n_dp,)), dma((n_dp,)),
            dma((2 * n_plane,)), dma((2 * n_plane,)),
            vm(tq.shape[1:], BF16), dma((tq.shape[2] // HEAD_SIZE,)),
        ],
        compiler_params=pltpu.CompilerParams(
            collective_id=0, has_side_effects=True, vmem_limit_bytes=VMEM_BYTES
        ),
    )(*args)
    return pl.pallas_call(
        write_out,
        out_shape=shapes,
        in_specs=[pl.BlockSpec(memory_space=pl.ANY)] * 4,
        out_specs=[pl.BlockSpec(memory_space=pl.ANY)] * 4,
        scratch_shapes=[vm(shape.shape, shape.dtype) for shape in shapes] + [dma((3 + PIECES,))] * 2,
        compiler_params=pltpu.CompilerParams(vmem_limit_bytes=VMEM_BYTES),
    )(*results)


def solution(mesh):
    rows = P(("grp", "dp"), "seq", None)
    return jax.shard_map(
        functools.partial(on_device, dict(mesh.shape)),
        mesh=mesh,
        in_specs=(rows, rows, rows, P(), P(), P(), rows, rows, rows, P(("grp", "dp"), "seq")),
        out_specs=(rows, P("dp", None), P(None, "dp"), P(None, "dp")),
        check_vma=False,
    )
```

```python
import functools

import jax
import jax.numpy as jnp
from jax import lax
from jax.experimental import pallas as pl
from jax.experimental.pallas import tpu as pltpu
from jax.sharding import PartitionSpec as P

MESH = pl.DeviceIdType.MESH
HEAD_SIZE = 128
F = 64
LANES = 128
ROWS = 8
ADAPTER_SCALE = 2.0
MASKED = -1e30
VMEM_BYTES = 67043328
PIECES = 4
EARLY_PAIRS = 2
EARLY_HEADS = 4
STAGES = (1, 5, 12)
LOG2E = 1.4426950408889634
BF16 = jnp.bfloat16
F32 = jnp.float32


def dot(a, b, dims=((1,), (0,))):
    return lax.dot_general(a, b, (dims, ((), ())), preferred_element_type=F32)


class Plan:
    def __init__(self, n_grp, n_dp, n_seq, feature_shape, down_width, up_width):
        self.n_grp, self.n_dp, self.n_seq = n_grp, n_dp, n_seq
        self.plane = n_grp // 2 * n_seq
        self.feature_rows = feature_shape[0] // n_dp
        self.down_width, self.up_width = down_width // n_dp, up_width // n_dp
        halves = []
        pairs = max(1, self.feature_rows // 16)
        for block in range(pairs):
            for tile in range(feature_shape[1] // LANES):
                for row in range(block * 16, min(block * 16 + 16, self.feature_rows), ROWS):
                    halves.append((0, row, tile * LANES, LANES))
        for which, width in ((1, self.down_width), (2, self.up_width)):
            for begin in range(0, width, LANES):
                halves.append((which, 0, begin, min(LANES, width - begin)))
        self.halves = halves
        self.used = (len(halves) + 1) // 2
        step = 2 * self.plane
        self.per = -(-self.used // step)
        self.units = self.per * step

    def where(self, unit):
        core, rest = divmod(unit, self.plane * self.per)
        return (core,) + divmod(rest, self.per)


def kernel(
    plan,
    x_hbm, sq_hbm, cot_hbm, w_hbm, ad_hbm, au_hbm, tq_hbm, tk_hbm, tv_hbm, pos_hbm,
    out_hbm, all_hbm,
    x_ref, sq_ref, cot_ref, w_ref, ad_ref, au_ref, tq_ref, k_ref, v_ref, pos_ref,
    bias_ref, dq_ref, gf_ref, gd_ref, gu_ref,
    g_ref, r1_ref, s1_ref, r2_ref, s2_ref, r3_ref, s3_ref, p_ref,
    load_sem, kv_send, kv_recv, core_send, core_recv, plane_send, plane_recv,
    dp_send, dp_recv, all_send, all_recv, out_ref, out_sem, own_sem,
):
    n_dp, n_seq, n_grp, n_plane, per = plan.n_dp, plan.n_seq, plan.n_grp, plan.plane, plan.per
    grp, dp, seq = lax.axis_index("grp"), lax.axis_index("dp"), lax.axis_index("seq")
    core = lax.rem(grp, 2)
    mine = lax.div(grp, 2) * n_seq + seq

    def in_plane(index, which_core):
        return {"grp": lax.div(index, n_seq) * 2 + which_core, "dp": dp, "seq": lax.rem(index, n_seq)}

    loads = []
    for n, (src, dst) in enumerate(
        (
            (pos_hbm, pos_ref.at[0]), (tk_hbm.at[0], k_ref.at[0]), (tv_hbm.at[0], v_ref.at[0]),
            (w_hbm, w_ref), (sq_hbm.at[0], sq_ref), (cot_hbm.at[0], cot_ref), (ad_hbm, ad_ref),
            (x_hbm.at[0], x_ref), (au_hbm, au_ref), (tq_hbm.at[0], tq_ref),
        )
    ):
        copy = pltpu.make_async_copy(src, dst, load_sem.at[n])
        copy.start()
        loads.append(copy)

    barrier = pltpu.get_barrier_semaphore()
    greeted = 0
    for j in range(1, n_plane):
        for other in range(2):
            pl.semaphore_signal(
                barrier, inc=1, device_id=in_plane(lax.rem(mine + j, n_plane), other), device_id_type=MESH
            )
            greeted += 1
    partner = {"grp": grp + 1 - 2 * core, "dp": dp, "seq": seq}
    pl.semaphore_signal(barrier, inc=1, device_id=partner, device_id_type=MESH)
    for j in range(1, n_dp):
        pl.semaphore_signal(
            barrier, inc=1, device_id={"grp": grp, "dp": lax.rem(dp + j, n_dp), "seq": seq}, device_id_type=MESH
        )
    greeted += n_dp

    for unit in range(plan.used, plan.units):
        c, p, k = plan.where(unit)
        g_ref[c, p, :, k] = jnp.zeros((n_dp, 16, LANES), BF16)

    rows = sq_ref.shape[0]
    lane = lax.broadcasted_iota(jnp.int32, (rows, LANES), 1)
    first = lane < F
    wide = lax.broadcasted_iota(jnp.int32, (2 * LANES, LANES), 1) < F
    depth = lax.broadcasted_iota(jnp.int32, (2 * LANES, LANES), 0)
    ones = ((lax.rem(depth, LANES) < F) == wide).astype(F32).astype(BF16)
    w_half = lax.broadcasted_iota(jnp.int32, (HEAD_SIZE, LANES), 1) < F

    def half_max(values):
        one = jnp.max(jnp.where(first, values, -jnp.inf), axis=1, keepdims=True)
        two = jnp.max(jnp.where(first, -jnp.inf, values), axis=1, keepdims=True)
        return jnp.where(first, one, two)

    def half_sum(values):
        stack = jnp.concatenate(values, axis=0)
        high = stack.astype(BF16)
        low = (stack - high.astype(F32)).astype(BF16)
        sums = dot(jnp.concatenate([high, low], axis=1), ones)
        return [sums[n * rows:(n + 1) * rows] for n in range(len(values))]

    kv_copies = []

    def send_keys():
        for n in range(3):
            loads[n].wait()
        pl.semaphore_wait(barrier, greeted)

        for n, ref in enumerate((pos_ref, k_ref, v_ref)):
            for j in range(1, n_seq):
                copy = pltpu.make_async_remote_copy(
                    src_ref=ref.at[0], dst_ref=ref.at[j],
                    send_sem=kv_send.at[n, j], recv_sem=kv_recv.at[n, j],
                    device_id={"grp": grp, "dp": dp, "seq": lax.rem(seq + j, n_seq)}, device_id_type=MESH,
                )
                copy.start()
                kv_copies.append(copy)

    for n in range(3, 6):
        loads[n].wait()
    for j in range(w_ref.shape[1] // LANES):
        if j == EARLY_PAIRS:
            send_keys()
        q2 = sq_ref[:, 2 * LANES * j:2 * LANES * (j + 1)]
        w = w_ref[:, LANES * j:LANES * (j + 1)].astype(F32)
        w2 = jnp.concatenate([jnp.where(w_half, w, 0.0), jnp.where(w_half, 0.0, w)], axis=0).astype(BF16)
        logit = dot(q2, w2)
        plus = jnp.exp(logit - half_max(logit))
        minus = jnp.exp(-logit - half_max(-logit))
        cot_a = cot_ref[:, 2 * LANES * j:2 * LANES * j + LANES].astype(F32)
        cot_b = cot_ref[:, 2 * LANES * j + LANES:2 * LANES * (j + 1)].astype(F32)
        cot_plus = jnp.where(first, cot_a, pltpu.roll(cot_b, F, 1))
        cot_minus = jnp.where(first, pltpu.roll(cot_a, F, 1), cot_b)
        sum_p, sum_m, sum_pc, sum_mc = half_sum([plus, minus, plus * cot_plus, minus * cot_minus])
        inv_p, inv_m = 1.0 / sum_p, 1.0 / sum_m
        dlogit = plus * inv_p * (cot_plus - sum_pc * inv_p) - minus * inv_m * (cot_minus - sum_mc * inv_m)
        dlogit_b = dlogit.astype(BF16)
        grad = dot(q2, dlogit_b, ((0,), (0,)))
        gf_ref[:, LANES * j:LANES * (j + 1)] = jnp.where(w_half, grad[:HEAD_SIZE], grad[HEAD_SIZE:])
        dq_ref[:, 2 * LANES * j:2 * LANES * (j + 1)] = dot(dlogit_b, w2, ((1,), (1,))).astype(BF16)
    for n in range(6, 9):
        loads[n].wait()
    x = x_ref[...]
    dq = dq_ref[...]
    down_act = dot(x, ad_ref[...], ((1,), (1,))).astype(BF16)
    dlow = (ADAPTER_SCALE * dot(dq, au_ref[...], ((1,), (1,)))).astype(BF16)
    gu_ref[...] = ADAPTER_SCALE * dot(down_act, dq, ((0,), (0,)))
    gd_ref[...] = dot(dlow, x, ((0,), (0,)))

    def half_unit(index, d):
        if index >= len(plan.halves):
            return jnp.zeros((ROWS, LANES), F32)
        which, row, begin, width = plan.halves[index]
        if which == 0:
            row = d * plan.feature_rows + row
            return gf_ref[row:row + ROWS, begin:begin + LANES]
        ref, own = ((gd_ref, plan.down_width), (gu_ref, plan.up_width))[which - 1]
        begin = d * own + begin
        value = ref[:, begin:begin + width]
        if width < LANES:
            value = jnp.concatenate([value, jnp.zeros((ROWS, LANES - width), F32)], axis=1)
        return value

    for unit in range(plan.used):
        c, p, k = plan.where(unit)
        for d in range(n_dp):
            g_ref[c, p, d, k] = jnp.concatenate(
                [half_unit(2 * unit, d), half_unit(2 * unit + 1, d)], axis=0
            ).astype(BF16)

    core_copy = pltpu.make_async_remote_copy(
        src_ref=g_ref.at[1 - core], dst_ref=r1_ref, send_sem=core_send, recv_sem=core_recv,
        device_id=partner, device_id_type=MESH,
    )
    core_copy.start()
    pending = []
    own_piece = pltpu.make_async_copy(s3_ref, all_hbm.at[core, mine], own_sem)

    def plane_stage():
        core_copy.wait_recv()
        s1_ref[...] = (g_ref[core].astype(F32) + r1_ref[...].astype(F32)).astype(BF16)
        for j in range(1, n_plane):
            other = lax.rem(mine + j, n_plane)
            copy = pltpu.make_async_remote_copy(
                src_ref=s1_ref.at[other], dst_ref=r2_ref.at[j],
                send_sem=plane_send.at[j], recv_sem=plane_recv.at[j],
                device_id=in_plane(other, core), device_id_type=MESH,
            )
            copy.start()
            pending.append(copy)

    def dp_stage():
        total = s1_ref[mine].astype(F32)
        for j in range(1, n_plane):
            pending[j - 1].wait_recv()
            total = total + r2_ref[j].astype(F32)
        s2_ref[...] = total.astype(BF16)
        for j in range(1, n_dp):
            other = lax.rem(dp + j, n_dp)
            copy = pltpu.make_async_remote_copy(
                src_ref=s2_ref.at[other], dst_ref=r3_ref.at[j],
                send_sem=dp_send.at[j], recv_sem=dp_recv.at[j],
                device_id={"grp": grp, "dp": other, "seq": seq}, device_id_type=MESH,
            )
            copy.start()
            pending.append(copy)

    def gather_stage():
        total = s2_ref[dp].astype(F32)
        for j in range(1, n_dp):
            pending[n_plane - 1 + j - 1].wait_recv()
            total = total + r3_ref[j].astype(F32)
        s3_ref[...] = total.astype(BF16)
        own_piece.start()
        for j in range(n_plane):
            for flip in range(2):
                if j == 0 and flip == 0:
                    continue
                copy = pltpu.make_async_remote_copy(
                    src_ref=s3_ref, dst_ref=all_hbm.at[core, mine],
                    send_sem=all_send.at[2 * j + flip], recv_sem=all_recv.at[2 * j + flip],
                    device_id=in_plane(lax.rem(mine + j, n_plane), core + flip * (1 - 2 * core)),
                    device_id_type=MESH,
                )
                copy.start()
                pending.append(copy)

    for copy in kv_copies[:2 * (n_seq - 1)]:
        copy.wait_recv()
    loads[9].wait()
    queries = tq_ref.shape[0]
    keys = k_ref.shape[1]
    own_pos = pos_ref[0].astype(F32)
    for begin in range(0, queries, LANES):
        column = jnp.transpose(jnp.broadcast_to(own_pos[:, begin:begin + LANES], (LANES, LANES)))
        for j in range(n_seq):
            key_pos = pos_ref[j].astype(F32)
            for at in range(0, keys, LANES):
                bias_ref[begin:begin + LANES, j * keys + at:j * keys + at + LANES] = jnp.where(
                    key_pos[:, at:at + LANES] <= column, 0.0, MASKED
                )
    heads = tq_ref.shape[1] // HEAD_SIZE
    group = heads // (k_ref.shape[2] // HEAD_SIZE)
    factor = HEAD_SIZE ** (-0.5) * LOG2E
    stages = dict(zip(STAGES, (plane_stage, dp_stage, gather_stage)))
    ones_v = jnp.ones((n_seq * keys, HEAD_SIZE), BF16)
    outs = []

    def weights(h):
        at = h // group * HEAD_SIZE
        k_all = k_ref[:, :, at:at + HEAD_SIZE].reshape(n_seq * keys, HEAD_SIZE)
        score = dot(tq_ref[:, h * HEAD_SIZE:(h + 1) * HEAD_SIZE], k_all, ((1,), (1,))) + bias_ref[...]
        top = jnp.max(score, axis=1, keepdims=True)
        return jnp.exp2((score - top) * factor).astype(BF16)

    def mix(h, weight):
        at = h // group * HEAD_SIZE
        v_all = jnp.concatenate(
            [v_ref[:, :, at:at + HEAD_SIZE].reshape(n_seq * keys, HEAD_SIZE), ones_v], axis=1
        )
        mixed = dot(weight, v_all)
        own = pl.ds(h * HEAD_SIZE, HEAD_SIZE)
        out_ref[:, own] = (mixed[:, :HEAD_SIZE] / mixed[:, HEAD_SIZE:]).astype(BF16)
        if outs:
            outs[-1].start()
        outs.append(pltpu.make_async_copy(out_ref.at[:, own], out_hbm.at[0, :, own], out_sem.at[h]))

    for h in range(heads):
        if h in stages:
            stages[h]()
        if h < EARLY_HEADS:
            p_ref[h] = weights(h)
        else:
            if h == EARLY_HEADS:
                for copy in kv_copies[2 * (n_seq - 1):]:
                    copy.wait_recv()
                for early in range(EARLY_HEADS):
                    mix(early, p_ref[early])
            mix(h, weights(h))
    outs[-1].start()

    for copy in pending[n_plane - 1 + n_dp - 1:]:
        copy.wait_recv()
    own_piece.wait()
    for copy in outs:
        copy.wait()
    core_copy.wait_send()
    for copy in kv_copies + pending:
        copy.wait_send()


def write_out(plan, out_hbm, all_hbm, out, gf_out, gd_out, gu_out,
              out_vm, all_vm, gf_vm, gd_vm, gu_vm, load_sem, store_sem):
    rows = out_vm.shape[1] // PIECES
    parts = [(0, pl.ds(piece * rows, rows)) for piece in range(PIECES)]
    gathered = pltpu.make_async_copy(all_hbm, all_vm, load_sem.at[PIECES])
    gathered.start()
    loads = [
        pltpu.make_async_copy(out_hbm.at[at], out_vm.at[at], load_sem.at[i]) for i, at in enumerate(parts)
    ]
    stores = [
        pltpu.make_async_copy(out_vm.at[at], out.at[at], store_sem.at[i]) for i, at in enumerate(parts)
    ]
    for load in loads:
        load.start()
    gathered.wait()
    for index, (which, row, begin, width) in enumerate(plan.halves):
        half = index % 2 * ROWS
        value = all_vm[plan.where(index // 2)].astype(F32)[half:half + ROWS, :width]
        (gf_vm, gd_vm, gu_vm)[which][row:row + ROWS, begin:begin + width] = value
    for load, store in zip(loads, stores):
        load.wait()
        store.start()
    for n, (held, target) in enumerate(((gf_vm, gf_out), (gd_vm, gd_out), (gu_vm, gu_out))):
        stores.append(pltpu.make_async_copy(held, target, store_sem.at[PIECES + n]))
        stores[-1].start()
    for store in stores:
        store.wait()


def on_device(mesh_shape, *args):
    x, sq, cot, w, ad, au, tq, tk, tv, pos = args
    n_grp, n_dp, n_seq = mesh_shape["grp"], mesh_shape["dp"], mesh_shape["seq"]
    plan = Plan(n_grp, n_dp, n_seq, w.shape, x.shape[2], sq.shape[2])
    n_plane, per = plan.plane, plan.per
    rows, queries, keys = sq.shape[1], tq.shape[1], tk.shape[1]
    vm, dma = pltpu.VMEM, pltpu.SemaphoreType.DMA
    unit = (16, LANES)
    shapes = (
        jax.ShapeDtypeStruct(tq.shape, BF16),
        jax.ShapeDtypeStruct((plan.feature_rows, w.shape[1]), F32),
        jax.ShapeDtypeStruct((ad.shape[0], plan.down_width), F32),
        jax.ShapeDtypeStruct((au.shape[0], plan.up_width), F32),
    )
    results = pl.pallas_call(
        functools.partial(kernel, plan),
        out_shape=(shapes[0], jax.ShapeDtypeStruct((2, n_plane, per) + unit, BF16)),
        in_specs=[pl.BlockSpec(memory_space=pl.ANY)] * 10,
        out_specs=[pl.BlockSpec(memory_space=pl.ANY)] * 2,
        scratch_shapes=[
            vm(x.shape[1:], BF16), vm(sq.shape[1:], BF16), vm(cot.shape[1:], BF16), vm(w.shape, BF16),
            vm(ad.shape, BF16), vm(au.shape, BF16), vm(tq.shape[1:], BF16),
            vm((n_seq, keys, tk.shape[2]), BF16), vm((n_seq, keys, tv.shape[2]), BF16),
            vm((n_seq, 1, keys), jnp.int32),
            vm((queries, n_seq * keys), F32), vm((rows, sq.shape[2]), BF16),
            vm(w.shape, F32), vm(ad.shape, F32), vm(au.shape, F32),
            vm((2, n_plane, n_dp, per) + unit, BF16),
            vm((n_plane, n_dp, per) + unit, BF16), vm((n_plane, n_dp, per) + unit, BF16),
            vm((n_plane, n_dp, per) + unit, BF16),
            vm((n_dp, per) + unit, BF16), vm((n_dp, per) + unit, BF16),
            vm((per,) + unit, BF16), vm((EARLY_HEADS, queries, n_seq * keys), BF16),
            dma((10,)), dma((3, n_seq)), dma((3, n_seq)), dma, dma,
            dma((n_plane,)), dma((n_plane,)), dma((n_dp,)), dma((n_dp,)),
            dma((2 * n_plane,)), dma((2 * n_plane,)),
            vm(tq.shape[1:], BF16), dma((tq.shape[2] // HEAD_SIZE,)), dma,
        ],
        compiler_params=pltpu.CompilerParams(
            collective_id=0, has_side_effects=True, vmem_limit_bytes=VMEM_BYTES
        ),
    )(*args)
    return pl.pallas_call(
        functools.partial(write_out, plan),
        out_shape=shapes,
        in_specs=[pl.BlockSpec(memory_space=pl.ANY)] * 2,
        out_specs=[pl.BlockSpec(memory_space=pl.ANY)] * 4,
        scratch_shapes=[vm(tq.shape, BF16), vm((2, n_plane, per) + unit, BF16)]
        + [vm(shape.shape, F32) for shape in shapes[1:]] + [dma((3 + PIECES,))] * 2,
        compiler_params=pltpu.CompilerParams(vmem_limit_bytes=VMEM_BYTES),
    )(*results)


def solution(mesh):
    rows = P(("grp", "dp"), "seq", None)
    return jax.shard_map(
        functools.partial(on_device, dict(mesh.shape)),
        mesh=mesh,
        in_specs=(rows, rows, rows, P(), P(), P(), rows, rows, rows, P(("grp", "dp"), "seq")),
        out_specs=(rows, P("dp", None), P(None, "dp"), P(None, "dp")),
        check_vma=False,
    )
```

```python
import functools

import jax
import jax.numpy as jnp
from jax import lax
from jax.experimental import pallas as pl
from jax.experimental.pallas import tpu as pltpu
from jax.sharding import PartitionSpec as P

MESH = pl.DeviceIdType.MESH
HEAD_SIZE = 128
F = 64
LANES = 128
ROWS = 8
ADAPTER_SCALE = 2.0
MASKED = -1e30
VMEM_BYTES = 67043328
PIECES = 4
EARLY_PAIRS = 2
PAIR_GROUP = 3
STAGES = (1, 13, 22)
LOG2E = 1.4426950408889634
BF16 = jnp.bfloat16
F32 = jnp.float32


def dot(a, b, dims=((1,), (0,))):
    return lax.dot_general(a, b, (dims, ((), ())), preferred_element_type=F32)


class Plan:
    def __init__(self, n_grp, n_dp, n_seq, feature_shape, down_width, up_width):
        self.n_grp, self.n_dp, self.n_seq = n_grp, n_dp, n_seq
        self.plane = n_grp // 2 * n_seq
        self.feature_rows = feature_shape[0] // n_dp
        self.down_width, self.up_width = down_width // n_dp, up_width // n_dp
        halves = []
        pairs = max(1, self.feature_rows // 16)
        for block in range(pairs):
            for tile in range(feature_shape[1] // LANES):
                for row in range(block * 16, min(block * 16 + 16, self.feature_rows), ROWS):
                    halves.append((0, row, tile * LANES, LANES))
        for which, width in ((1, self.down_width), (2, self.up_width)):
            for begin in range(0, width, LANES):
                halves.append((which, 0, begin, min(LANES, width - begin)))
        self.halves = halves
        self.used = (len(halves) + 1) // 2
        step = 2 * self.plane
        self.per = -(-self.used // step)
        self.units = self.per * step

    def where(self, unit):
        core, rest = divmod(unit, self.plane * self.per)
        return (core,) + divmod(rest, self.per)


def kernel(
    plan,
    x_hbm, sq_hbm, cot_hbm, w_hbm, ad_hbm, au_hbm, tq_hbm, tk_hbm, tv_hbm, pos_hbm,
    out_hbm, all_hbm,
    x_ref, sq_ref, cot_ref, w_ref, ad_ref, au_ref, tq_ref, k_ref, v_ref, pos_ref,
    bias_ref, dq_ref, gf_ref, gd_ref, gu_ref,
    g_ref, r1_ref, s1_ref, r2_ref, s2_ref, r3_ref, s3_ref, p_ref,
    load_sem, kv_send, kv_recv, core_send, core_recv, plane_send, plane_recv,
    dp_send, dp_recv, all_send, all_recv, out_ref, out_sem, own_sem,
):
    n_dp, n_seq, n_grp, n_plane, per = plan.n_dp, plan.n_seq, plan.n_grp, plan.plane, plan.per
    grp, dp, seq = lax.axis_index("grp"), lax.axis_index("dp"), lax.axis_index("seq")
    core = lax.rem(grp, 2)
    mine = lax.div(grp, 2) * n_seq + seq

    def in_plane(index, which_core):
        return {"grp": lax.div(index, n_seq) * 2 + which_core, "dp": dp, "seq": lax.rem(index, n_seq)}

    loads = []
    for n, (src, dst) in enumerate(
        (
            (w_hbm, w_ref), (sq_hbm.at[0], sq_ref), (cot_hbm.at[0], cot_ref),
            (pos_hbm, pos_ref.at[0]), (tk_hbm.at[0], k_ref.at[0]), (ad_hbm, ad_ref),
            (x_hbm.at[0], x_ref), (au_hbm, au_ref), (tv_hbm.at[0], v_ref.at[0]), (tq_hbm.at[0], tq_ref),
        )
    ):
        copy = pltpu.make_async_copy(src, dst, load_sem.at[n])
        copy.start()
        loads.append(copy)

    barrier = pltpu.get_barrier_semaphore()
    greeted = 0
    for j in range(1, n_plane):
        for other in range(2):
            pl.semaphore_signal(
                barrier, inc=1, device_id=in_plane(lax.rem(mine + j, n_plane), other), device_id_type=MESH
            )
            greeted += 1
    partner = {"grp": grp + 1 - 2 * core, "dp": dp, "seq": seq}
    pl.semaphore_signal(barrier, inc=1, device_id=partner, device_id_type=MESH)
    for j in range(1, n_dp):
        pl.semaphore_signal(
            barrier, inc=1, device_id={"grp": grp, "dp": lax.rem(dp + j, n_dp), "seq": seq}, device_id_type=MESH
        )
    greeted += n_dp

    for unit in range(plan.used, plan.units):
        c, p, k = plan.where(unit)
        g_ref[c, p, :, k] = jnp.zeros((n_dp, 16, LANES), BF16)

    rows = sq_ref.shape[0]
    lane = lax.broadcasted_iota(jnp.int32, (rows, LANES), 1)
    first = lane < F
    wide = lax.broadcasted_iota(jnp.int32, (2 * LANES, LANES), 1) < F
    depth = lax.broadcasted_iota(jnp.int32, (2 * LANES, LANES), 0)
    ones = ((lax.rem(depth, LANES) < F) == wide).astype(F32).astype(BF16)
    w_half = lax.broadcasted_iota(jnp.int32, (HEAD_SIZE, LANES), 1) < F

    def half_max(values):
        one = jnp.max(jnp.where(first, values, -jnp.inf), axis=1, keepdims=True)
        two = jnp.max(jnp.where(first, -jnp.inf, values), axis=1, keepdims=True)
        return jnp.where(first, one, two)

    def half_sum(values):
        stack = jnp.concatenate(values, axis=0)
        high = stack.astype(BF16)
        low = (stack - high.astype(F32)).astype(BF16)
        sums = dot(jnp.concatenate([high, low], axis=1), ones)
        return [sums[n * rows:(n + 1) * rows] for n in range(len(values))]

    kv_copies = []

    def send(first_array, *refs):
        for n, ref in enumerate(refs, first_array):
            for j in range(1, n_seq):
                copy = pltpu.make_async_remote_copy(
                    src_ref=ref.at[0], dst_ref=ref.at[j],
                    send_sem=kv_send.at[n, j], recv_sem=kv_recv.at[n, j],
                    device_id={"grp": grp, "dp": dp, "seq": lax.rem(seq + j, n_seq)}, device_id_type=MESH,
                )
                copy.start()
                kv_copies.append(copy)

    for n in range(3):
        loads[n].wait()
    def begin_pair(j):
        q2 = sq_ref[:, 2 * LANES * j:2 * LANES * (j + 1)]
        w = w_ref[:, LANES * j:LANES * (j + 1)].astype(F32)
        w2 = jnp.concatenate([jnp.where(w_half, w, 0.0), jnp.where(w_half, 0.0, w)], axis=0).astype(BF16)
        logit = dot(q2, w2)
        return q2, w2, logit

    def mid_pair(j, q2, w2, logit):
        plus = jnp.exp(logit - half_max(logit))
        minus = jnp.exp(-logit - half_max(-logit))
        cot_a = cot_ref[:, 2 * LANES * j:2 * LANES * j + LANES].astype(F32)
        cot_b = cot_ref[:, 2 * LANES * j + LANES:2 * LANES * (j + 1)].astype(F32)
        cot_plus = jnp.where(first, cot_a, pltpu.roll(cot_b, F, 1))
        cot_minus = jnp.where(first, pltpu.roll(cot_a, F, 1), cot_b)
        sums = half_sum([plus, minus, plus * cot_plus, minus * cot_minus])
        return q2, w2, plus, minus, cot_plus, cot_minus, sums

    def end_pair(j, q2, w2, plus, minus, cot_plus, cot_minus, sums):
        sum_p, sum_m, sum_pc, sum_mc = sums
        inv_p, inv_m = 1.0 / sum_p, 1.0 / sum_m
        dlogit = plus * inv_p * (cot_plus - sum_pc * inv_p) - minus * inv_m * (cot_minus - sum_mc * inv_m)
        dlogit_b = dlogit.astype(BF16)
        grad = dot(q2, dlogit_b, ((0,), (0,)))
        gf_ref[:, LANES * j:LANES * (j + 1)] = jnp.where(w_half, grad[:HEAD_SIZE], grad[HEAD_SIZE:])
        dq_ref[:, 2 * LANES * j:2 * LANES * (j + 1)] = dot(dlogit_b, w2, ((1,), (1,))).astype(BF16)

    def student_pairs(begin, end):
        states = [begin_pair(j) for j in range(begin, end)]
        states = [mid_pair(j, *state) for j, state in zip(range(begin, end), states)]
        for j, state in zip(range(begin, end), states):
            end_pair(j, *state)

    pairs = w_ref.shape[1] // LANES
    student_pairs(0, EARLY_PAIRS)
    for n in range(3, 5):
        loads[n].wait()
    pl.semaphore_wait(barrier, greeted)
    send(0, pos_ref, k_ref)
    for begin in range(EARLY_PAIRS, pairs, PAIR_GROUP):
        student_pairs(begin, min(begin + PAIR_GROUP, pairs))
    for n in range(5, 8):
        loads[n].wait()
    x = x_ref[...]
    dq = dq_ref[...]
    down_act = dot(x, ad_ref[...], ((1,), (1,))).astype(BF16)
    dlow = (ADAPTER_SCALE * dot(dq, au_ref[...], ((1,), (1,)))).astype(BF16)
    gu_ref[...] = ADAPTER_SCALE * dot(down_act, dq, ((0,), (0,)))
    gd_ref[...] = dot(dlow, x, ((0,), (0,)))

    def half_unit(index, d):
        if index >= len(plan.halves):
            return jnp.zeros((ROWS, LANES), F32)
        which, row, begin, width = plan.halves[index]
        if which == 0:
            row = d * plan.feature_rows + row
            return gf_ref[row:row + ROWS, begin:begin + LANES]
        ref, own = ((gd_ref, plan.down_width), (gu_ref, plan.up_width))[which - 1]
        begin = d * own + begin
        value = ref[:, begin:begin + width]
        if width < LANES:
            value = jnp.concatenate([value, jnp.zeros((ROWS, LANES - width), F32)], axis=1)
        return value

    for unit in range(plan.used):
        c, p, k = plan.where(unit)
        for d in range(n_dp):
            g_ref[c, p, d, k] = jnp.concatenate(
                [half_unit(2 * unit, d), half_unit(2 * unit + 1, d)], axis=0
            ).astype(BF16)

    core_copy = pltpu.make_async_remote_copy(
        src_ref=g_ref.at[1 - core], dst_ref=r1_ref, send_sem=core_send, recv_sem=core_recv,
        device_id=partner, device_id_type=MESH,
    )
    core_copy.start()
    pending = []
    own_piece = pltpu.make_async_copy(s3_ref, all_hbm.at[core, mine], own_sem)

    def plane_stage():
        core_copy.wait_recv()
        s1_ref[...] = (g_ref[core].astype(F32) + r1_ref[...].astype(F32)).astype(BF16)
        for j in range(1, n_plane):
            other = lax.rem(mine + j, n_plane)
            copy = pltpu.make_async_remote_copy(
                src_ref=s1_ref.at[other], dst_ref=r2_ref.at[j],
                send_sem=plane_send.at[j], recv_sem=plane_recv.at[j],
                device_id=in_plane(other, core), device_id_type=MESH,
            )
            copy.start()
            pending.append(copy)
        loads[8].wait()
        send(2, v_ref)

    def dp_stage():
        total = s1_ref[mine].astype(F32)
        for j in range(1, n_plane):
            pending[j - 1].wait_recv()
            total = total + r2_ref[j].astype(F32)
        s2_ref[...] = total.astype(BF16)
        for j in range(1, n_dp):
            other = lax.rem(dp + j, n_dp)
            copy = pltpu.make_async_remote_copy(
                src_ref=s2_ref.at[other], dst_ref=r3_ref.at[j],
                send_sem=dp_send.at[j], recv_sem=dp_recv.at[j],
                device_id={"grp": grp, "dp": other, "seq": seq}, device_id_type=MESH,
            )
            copy.start()
            pending.append(copy)

    def gather_stage():
        total = s2_ref[dp].astype(F32)
        for j in range(1, n_dp):
            pending[n_plane - 1 + j - 1].wait_recv()
            total = total + r3_ref[j].astype(F32)
        s3_ref[...] = total.astype(BF16)
        own_piece.start()
        for j in range(n_plane):
            for flip in range(2):
                if j == 0 and flip == 0:
                    continue
                copy = pltpu.make_async_remote_copy(
                    src_ref=s3_ref, dst_ref=all_hbm.at[core, mine],
                    send_sem=all_send.at[2 * j + flip], recv_sem=all_recv.at[2 * j + flip],
                    device_id=in_plane(lax.rem(mine + j, n_plane), core + flip * (1 - 2 * core)),
                    device_id_type=MESH,
                )
                copy.start()
                pending.append(copy)

    for copy in kv_copies[:2 * (n_seq - 1)]:
        copy.wait_recv()
    loads[9].wait()
    queries = tq_ref.shape[0]
    keys = k_ref.shape[1]
    own_pos = pos_ref[0].astype(F32)
    for begin in range(0, queries, LANES):
        column = jnp.transpose(jnp.broadcast_to(own_pos[:, begin:begin + LANES], (LANES, LANES)))
        for j in range(n_seq):
            key_pos = pos_ref[j].astype(F32)
            for at in range(0, keys, LANES):
                bias_ref[begin:begin + LANES, j * keys + at:j * keys + at + LANES] = jnp.where(
                    key_pos[:, at:at + LANES] <= column, 0.0, MASKED
                )
    heads = tq_ref.shape[1] // HEAD_SIZE
    group = heads // (k_ref.shape[2] // HEAD_SIZE)
    factor = HEAD_SIZE ** (-0.5) * LOG2E
    stages = dict(zip(STAGES, (plane_stage, dp_stage, gather_stage)))
    ones_v = jnp.ones((n_seq * keys, HEAD_SIZE), BF16)
    outs = []

    def weights(h):
        at = h // group * HEAD_SIZE
        k_all = k_ref[:, :, at:at + HEAD_SIZE].reshape(n_seq * keys, HEAD_SIZE)
        score = dot(tq_ref[:, h * HEAD_SIZE:(h + 1) * HEAD_SIZE], k_all, ((1,), (1,))) + bias_ref[...]
        top = jnp.max(score, axis=1, keepdims=True)
        return jnp.exp2((score - top) * factor).astype(BF16)

    def mix(h, weight):
        at = h // group * HEAD_SIZE
        v_all = jnp.concatenate(
            [v_ref[:, :, at:at + HEAD_SIZE].reshape(n_seq * keys, HEAD_SIZE), ones_v], axis=1
        )
        mixed = dot(weight, v_all)
        own = pl.ds(h * HEAD_SIZE, HEAD_SIZE)
        out_ref[:, own] = (mixed[:, :HEAD_SIZE] / mixed[:, HEAD_SIZE:]).astype(BF16)
        if outs:
            outs[-1].start()
        outs.append(pltpu.make_async_copy(out_ref.at[:, own], out_hbm.at[0, :, own], out_sem.at[h]))

    for step in range(2 * heads):
        if step in stages:
            stages[step]()
        if step == heads:
            for copy in kv_copies[2 * (n_seq - 1):]:
                copy.wait_recv()
        if step < heads:
            p_ref[step] = weights(step)
        else:
            mix(step - heads, p_ref[step - heads])
    outs[-1].start()

    for copy in pending[n_plane - 1 + n_dp - 1:]:
        copy.wait_recv()
    own_piece.wait()
    for copy in outs:
        copy.wait()
    core_copy.wait_send()
    for copy in kv_copies + pending:
        copy.wait_send()


def write_out(plan, out_hbm, all_hbm, out, gf_out, gd_out, gu_out,
              out_vm, all_vm, gf_vm, gd_vm, gu_vm, load_sem, store_sem):
    rows = out_vm.shape[1] // PIECES
    parts = [(0, pl.ds(piece * rows, rows)) for piece in range(PIECES)]
    gathered = pltpu.make_async_copy(all_hbm, all_vm, load_sem.at[PIECES])
    gathered.start()
    loads = [
        pltpu.make_async_copy(out_hbm.at[at], out_vm.at[at], load_sem.at[i]) for i, at in enumerate(parts)
    ]
    stores = [
        pltpu.make_async_copy(out_vm.at[at], out.at[at], store_sem.at[i]) for i, at in enumerate(parts)
    ]
    for load in loads:
        load.start()
    gathered.wait()
    for index, (which, row, begin, width) in enumerate(plan.halves):
        half = index % 2 * ROWS
        value = all_vm[plan.where(index // 2)].astype(F32)[half:half + ROWS, :width]
        (gf_vm, gd_vm, gu_vm)[which][row:row + ROWS, begin:begin + width] = value
    for load, store in zip(loads, stores):
        load.wait()
        store.start()
    for n, (held, target) in enumerate(((gf_vm, gf_out), (gd_vm, gd_out), (gu_vm, gu_out))):
        stores.append(pltpu.make_async_copy(held, target, store_sem.at[PIECES + n]))
        stores[-1].start()
    for store in stores:
        store.wait()


def on_device(mesh_shape, *args):
    x, sq, cot, w, ad, au, tq, tk, tv, pos = args
    n_grp, n_dp, n_seq = mesh_shape["grp"], mesh_shape["dp"], mesh_shape["seq"]
    plan = Plan(n_grp, n_dp, n_seq, w.shape, x.shape[2], sq.shape[2])
    n_plane, per = plan.plane, plan.per
    rows, queries, keys = sq.shape[1], tq.shape[1], tk.shape[1]
    vm, dma = pltpu.VMEM, pltpu.SemaphoreType.DMA
    unit = (16, LANES)
    shapes = (
        jax.ShapeDtypeStruct(tq.shape, BF16),
        jax.ShapeDtypeStruct((plan.feature_rows, w.shape[1]), F32),
        jax.ShapeDtypeStruct((ad.shape[0], plan.down_width), F32),
        jax.ShapeDtypeStruct((au.shape[0], plan.up_width), F32),
    )
    results = pl.pallas_call(
        functools.partial(kernel, plan),
        out_shape=(shapes[0], jax.ShapeDtypeStruct((2, n_plane, per) + unit, BF16)),
        in_specs=[pl.BlockSpec(memory_space=pl.ANY)] * 10,
        out_specs=[pl.BlockSpec(memory_space=pl.ANY)] * 2,
        scratch_shapes=[
            vm(x.shape[1:], BF16), vm(sq.shape[1:], BF16), vm(cot.shape[1:], BF16), vm(w.shape, BF16),
            vm(ad.shape, BF16), vm(au.shape, BF16), vm(tq.shape[1:], BF16),
            vm((n_seq, keys, tk.shape[2]), BF16), vm((n_seq, keys, tv.shape[2]), BF16),
            vm((n_seq, 1, keys), jnp.int32),
            vm((queries, n_seq * keys), F32), vm((rows, sq.shape[2]), BF16),
            vm(w.shape, F32), vm(ad.shape, F32), vm(au.shape, F32),
            vm((2, n_plane, n_dp, per) + unit, BF16),
            vm((n_plane, n_dp, per) + unit, BF16), vm((n_plane, n_dp, per) + unit, BF16),
            vm((n_plane, n_dp, per) + unit, BF16),
            vm((n_dp, per) + unit, BF16), vm((n_dp, per) + unit, BF16),
            vm((per,) + unit, BF16), vm((tq.shape[2] // HEAD_SIZE, queries, n_seq * keys), BF16),
            dma((10,)), dma((3, n_seq)), dma((3, n_seq)), dma, dma,
            dma((n_plane,)), dma((n_plane,)), dma((n_dp,)), dma((n_dp,)),
            dma((2 * n_plane,)), dma((2 * n_plane,)),
            vm(tq.shape[1:], BF16), dma((tq.shape[2] // HEAD_SIZE,)), dma,
        ],
        compiler_params=pltpu.CompilerParams(
            collective_id=0, has_side_effects=True, vmem_limit_bytes=VMEM_BYTES
        ),
    )(*args)
    return pl.pallas_call(
        functools.partial(write_out, plan),
        out_shape=shapes,
        in_specs=[pl.BlockSpec(memory_space=pl.ANY)] * 2,
        out_specs=[pl.BlockSpec(memory_space=pl.ANY)] * 4,
        scratch_shapes=[vm(tq.shape, BF16), vm((2, n_plane, per) + unit, BF16)]
        + [vm(shape.shape, F32) for shape in shapes[1:]] + [dma((3 + PIECES,))] * 2,
        compiler_params=pltpu.CompilerParams(vmem_limit_bytes=VMEM_BYTES),
    )(*results)


def solution(mesh):
    rows = P(("grp", "dp"), "seq", None)
    return jax.shard_map(
        functools.partial(on_device, dict(mesh.shape)),
        mesh=mesh,
        in_specs=(rows, rows, rows, P(), P(), P(), rows, rows, rows, P(("grp", "dp"), "seq")),
        out_specs=(rows, P("dp", None), P(None, "dp"), P(None, "dp")),
        check_vma=False,
    )
```

```python
import functools

import jax
import jax.numpy as jnp
from jax import lax
from jax.experimental import pallas as pl
from jax.experimental.pallas import tpu as pltpu
from jax.sharding import PartitionSpec as P

MESH = pl.DeviceIdType.MESH
HEAD_SIZE = 128
F = 64
LANES = 128
ROWS = 8
ADAPTER_SCALE = 2.0
MASKED = -1e30
VMEM_BYTES = 67043328
PIECES = 4
EARLY_PAIRS = 2
PAIR_GROUP = 3
STAGES = (12, 24)
LOG2E = 1.4426950408889634
BF16 = jnp.bfloat16
F32 = jnp.float32


def dot(a, b, dims=((1,), (0,))):
    return lax.dot_general(a, b, (dims, ((), ())), preferred_element_type=F32)


class Plan:
    def __init__(self, n_grp, n_dp, n_seq, feature_shape, down_width, up_width):
        self.n_grp, self.n_dp, self.n_seq = n_grp, n_dp, n_seq
        self.plane = n_grp // 2 * n_seq
        self.feature_rows = feature_shape[0] // n_dp
        self.down_width, self.up_width = down_width // n_dp, up_width // n_dp
        halves = []
        pairs = max(1, self.feature_rows // 16)
        for block in range(pairs):
            for tile in range(feature_shape[1] // LANES):
                for row in range(block * 16, min(block * 16 + 16, self.feature_rows), ROWS):
                    halves.append((0, row, tile * LANES, LANES))
        for which, width in ((1, self.down_width), (2, self.up_width)):
            for begin in range(0, width, LANES):
                halves.append((which, 0, begin, min(LANES, width - begin)))
        self.halves = halves
        self.used = (len(halves) + 1) // 2
        step = 2 * self.plane
        self.per = -(-self.used // step)
        self.units = self.per * step

    def where(self, unit):
        core, rest = divmod(unit, self.plane * self.per)
        return (core,) + divmod(rest, self.per)


def kernel(
    plan,
    x_hbm, sq_hbm, cot_hbm, w_hbm, ad_hbm, au_hbm, tq_hbm, tk_hbm, tv_hbm, pos_hbm,
    out_hbm, all_hbm,
    x_ref, sq_ref, cot_ref, w_ref, ad_ref, au_ref, tq_ref, k_ref, v_ref, pos_ref,
    bias_ref, dq_ref, gf_ref, gd_ref, gu_ref,
    g_ref, r1_ref, s1_ref, r2_ref, s2_ref, r3_ref, s3_ref, p_ref,
    load_sem, kv_send, kv_recv, core_send, core_recv, plane_send, plane_recv,
    dp_send, dp_recv, all_send, all_recv, out_ref, out_sem, own_sem,
):
    n_dp, n_seq, n_grp, n_plane, per = plan.n_dp, plan.n_seq, plan.n_grp, plan.plane, plan.per
    grp, dp, seq = lax.axis_index("grp"), lax.axis_index("dp"), lax.axis_index("seq")
    core = lax.rem(grp, 2)
    mine = lax.div(grp, 2) * n_seq + seq

    def in_plane(index, which_core):
        return {"grp": lax.div(index, n_seq) * 2 + which_core, "dp": dp, "seq": lax.rem(index, n_seq)}

    loads = []
    for n, (src, dst) in enumerate(
        (
            (w_hbm, w_ref), (sq_hbm.at[0], sq_ref), (cot_hbm.at[0], cot_ref),
            (pos_hbm, pos_ref.at[0]), (tk_hbm.at[0], k_ref.at[0]), (ad_hbm, ad_ref),
            (x_hbm.at[0], x_ref), (au_hbm, au_ref), (tv_hbm.at[0], v_ref.at[0]), (tq_hbm.at[0], tq_ref),
        )
    ):
        copy = pltpu.make_async_copy(src, dst, load_sem.at[n])
        copy.start()
        loads.append(copy)

    barrier = pltpu.get_barrier_semaphore()
    greeted = 0
    for j in range(1, n_plane):
        for other in range(2):
            pl.semaphore_signal(
                barrier, inc=1, device_id=in_plane(lax.rem(mine + j, n_plane), other), device_id_type=MESH
            )
            greeted += 1
    partner = {"grp": grp + 1 - 2 * core, "dp": dp, "seq": seq}
    pl.semaphore_signal(barrier, inc=1, device_id=partner, device_id_type=MESH)
    for j in range(1, n_dp):
        pl.semaphore_signal(
            barrier, inc=1, device_id={"grp": grp, "dp": lax.rem(dp + j, n_dp), "seq": seq}, device_id_type=MESH
        )
    greeted += n_dp

    for unit in range(plan.used, plan.units):
        c, p, k = plan.where(unit)
        g_ref[c, p, :, k] = jnp.zeros((n_dp, 16, LANES), BF16)

    rows = sq_ref.shape[0]
    lane = lax.broadcasted_iota(jnp.int32, (rows, LANES), 1)
    first = lane < F
    wide = lax.broadcasted_iota(jnp.int32, (2 * LANES, LANES), 1) < F
    depth = lax.broadcasted_iota(jnp.int32, (2 * LANES, LANES), 0)
    ones = ((lax.rem(depth, LANES) < F) == wide).astype(F32).astype(BF16)
    w_half = lax.broadcasted_iota(jnp.int32, (HEAD_SIZE, LANES), 1) < F

    def half_max(values):
        one = jnp.max(jnp.where(first, values, -jnp.inf), axis=1, keepdims=True)
        two = jnp.max(jnp.where(first, -jnp.inf, values), axis=1, keepdims=True)
        return jnp.where(first, one, two)

    def half_sum(values):
        stack = jnp.concatenate(values, axis=0)
        high = stack.astype(BF16)
        low = (stack - high.astype(F32)).astype(BF16)
        sums = dot(jnp.concatenate([high, low], axis=1), ones)
        return [sums[n * rows:(n + 1) * rows] for n in range(len(values))]

    kv_copies = []

    def send(first_array, *refs):
        for n, ref in enumerate(refs, first_array):
            for j in range(1, n_seq):
                copy = pltpu.make_async_remote_copy(
                    src_ref=ref.at[0], dst_ref=ref.at[j],
                    send_sem=kv_send.at[n, j], recv_sem=kv_recv.at[n, j],
                    device_id={"grp": grp, "dp": dp, "seq": lax.rem(seq + j, n_seq)}, device_id_type=MESH,
                )
                copy.start()
                kv_copies.append(copy)

    for n in range(3):
        loads[n].wait()
    def begin_pair(j):
        q2 = sq_ref[:, 2 * LANES * j:2 * LANES * (j + 1)]
        w = w_ref[:, LANES * j:LANES * (j + 1)].astype(F32)
        w2 = jnp.concatenate([jnp.where(w_half, w, 0.0), jnp.where(w_half, 0.0, w)], axis=0).astype(BF16)
        logit = dot(q2, w2)
        return q2, w2, logit

    def mid_pair(j, q2, w2, logit):
        plus = jnp.exp(logit - half_max(logit))
        minus = jnp.exp(-logit - half_max(-logit))
        cot_a = cot_ref[:, 2 * LANES * j:2 * LANES * j + LANES].astype(F32)
        cot_b = cot_ref[:, 2 * LANES * j + LANES:2 * LANES * (j + 1)].astype(F32)
        cot_plus = jnp.where(first, cot_a, pltpu.roll(cot_b, F, 1))
        cot_minus = jnp.where(first, pltpu.roll(cot_a, F, 1), cot_b)
        sums = half_sum([plus, minus, plus * cot_plus, minus * cot_minus])
        return q2, w2, plus, minus, cot_plus, cot_minus, sums

    def end_pair(j, q2, w2, plus, minus, cot_plus, cot_minus, sums):
        sum_p, sum_m, sum_pc, sum_mc = sums
        inv_p, inv_m = 1.0 / sum_p, 1.0 / sum_m
        dlogit = plus * inv_p * (cot_plus - sum_pc * inv_p) - minus * inv_m * (cot_minus - sum_mc * inv_m)
        dlogit_b = dlogit.astype(BF16)
        grad = dot(q2, dlogit_b, ((0,), (0,)))
        gf_ref[:, LANES * j:LANES * (j + 1)] = jnp.where(w_half, grad[:HEAD_SIZE], grad[HEAD_SIZE:])
        dq_ref[:, 2 * LANES * j:2 * LANES * (j + 1)] = dot(dlogit_b, w2, ((1,), (1,))).astype(BF16)

    def student_pairs(begin, end):
        states = [begin_pair(j) for j in range(begin, end)]
        states = [mid_pair(j, *state) for j, state in zip(range(begin, end), states)]
        for j, state in zip(range(begin, end), states):
            end_pair(j, *state)

    pairs = w_ref.shape[1] // LANES
    student_pairs(0, EARLY_PAIRS)
    for n in range(3, 5):
        loads[n].wait()
    pl.semaphore_wait(barrier, greeted)
    send(0, pos_ref, k_ref)
    for begin in range(EARLY_PAIRS, pairs, PAIR_GROUP):
        student_pairs(begin, min(begin + PAIR_GROUP, pairs))
    for n in range(5, 8):
        loads[n].wait()
    x = x_ref[...]
    dq = dq_ref[...]
    down_act = dot(x, ad_ref[...], ((1,), (1,))).astype(BF16)
    dlow = (ADAPTER_SCALE * dot(dq, au_ref[...], ((1,), (1,)))).astype(BF16)
    gu_ref[...] = ADAPTER_SCALE * dot(down_act, dq, ((0,), (0,)))
    gd_ref[...] = dot(dlow, x, ((0,), (0,)))

    def half_unit(index, d):
        if index >= len(plan.halves):
            return jnp.zeros((ROWS, LANES), F32)
        which, row, begin, width = plan.halves[index]
        if which == 0:
            row = d * plan.feature_rows + row
            return gf_ref[row:row + ROWS, begin:begin + LANES]
        ref, own = ((gd_ref, plan.down_width), (gu_ref, plan.up_width))[which - 1]
        begin = d * own + begin
        value = ref[:, begin:begin + width]
        if width < LANES:
            value = jnp.concatenate([value, jnp.zeros((ROWS, LANES - width), F32)], axis=1)
        return value

    for unit in range(plan.used):
        c, p, k = plan.where(unit)
        for d in range(n_dp):
            g_ref[c, p, d, k] = jnp.concatenate(
                [half_unit(2 * unit, d), half_unit(2 * unit + 1, d)], axis=0
            ).astype(BF16)

    core_copy = pltpu.make_async_remote_copy(
        src_ref=g_ref.at[1 - core], dst_ref=r1_ref, send_sem=core_send, recv_sem=core_recv,
        device_id=partner, device_id_type=MESH,
    )
    core_copy.start()
    pending = []
    own_piece = pltpu.make_async_copy(s3_ref, all_hbm.at[core, mine], own_sem)

    def plane_stage():
        core_copy.wait_recv()
        s1_ref[...] = (g_ref[core].astype(F32) + r1_ref[...].astype(F32)).astype(BF16)
        for j in range(1, n_plane):
            other = lax.rem(mine + j, n_plane)
            copy = pltpu.make_async_remote_copy(
                src_ref=s1_ref.at[other], dst_ref=r2_ref.at[j],
                send_sem=plane_send.at[j], recv_sem=plane_recv.at[j],
                device_id=in_plane(other, core), device_id_type=MESH,
            )
            copy.start()
            pending.append(copy)
        loads[8].wait()
        send(2, v_ref)

    def dp_stage():
        total = s1_ref[mine].astype(F32)
        for j in range(1, n_plane):
            pending[j - 1].wait_recv()
            total = total + r2_ref[j].astype(F32)
        s2_ref[...] = total.astype(BF16)
        for j in range(1, n_dp):
            other = lax.rem(dp + j, n_dp)
            copy = pltpu.make_async_remote_copy(
                src_ref=s2_ref.at[other], dst_ref=r3_ref.at[j],
                send_sem=dp_send.at[j], recv_sem=dp_recv.at[j],
                device_id={"grp": grp, "dp": other, "seq": seq}, device_id_type=MESH,
            )
            copy.start()
            pending.append(copy)

    def gather_stage():
        total = s2_ref[dp].astype(F32)
        for j in range(1, n_dp):
            pending[n_plane - 1 + j - 1].wait_recv()
            total = total + r3_ref[j].astype(F32)
        s3_ref[...] = total.astype(BF16)
        own_piece.start()
        for j in range(n_plane):
            for flip in range(2):
                if j == 0 and flip == 0:
                    continue
                copy = pltpu.make_async_remote_copy(
                    src_ref=s3_ref, dst_ref=all_hbm.at[core, mine],
                    send_sem=all_send.at[2 * j + flip], recv_sem=all_recv.at[2 * j + flip],
                    device_id=in_plane(lax.rem(mine + j, n_plane), core + flip * (1 - 2 * core)),
                    device_id_type=MESH,
                )
                copy.start()
                pending.append(copy)

    plane_stage()

    for copy in kv_copies[:2 * (n_seq - 1)]:
        copy.wait_recv()
    loads[9].wait()
    queries = tq_ref.shape[0]
    keys = k_ref.shape[1]
    own_pos = pos_ref[0].astype(F32)
    for begin in range(0, queries, LANES):
        column = jnp.transpose(jnp.broadcast_to(own_pos[:, begin:begin + LANES], (LANES, LANES)))
        for j in range(n_seq):
            key_pos = pos_ref[j].astype(F32)
            for at in range(0, keys, LANES):
                bias_ref[begin:begin + LANES, j * keys + at:j * keys + at + LANES] = jnp.where(
                    key_pos[:, at:at + LANES] <= column, 0.0, MASKED
                )
    heads = tq_ref.shape[1] // HEAD_SIZE
    group = heads // (k_ref.shape[2] // HEAD_SIZE)
    factor = HEAD_SIZE ** (-0.5) * LOG2E
    stages = dict(zip(STAGES, (dp_stage, gather_stage)))
    ones_v = jnp.ones((n_seq * keys, HEAD_SIZE), BF16)
    outs = []

    def weights(h):
        at = h // group * HEAD_SIZE
        k_all = k_ref[:, :, at:at + HEAD_SIZE].reshape(n_seq * keys, HEAD_SIZE)
        score = dot(tq_ref[:, h * HEAD_SIZE:(h + 1) * HEAD_SIZE], k_all, ((1,), (1,))) + bias_ref[...]
        top = jnp.max(score, axis=1, keepdims=True)
        return jnp.exp2((score - top) * factor).astype(BF16)

    def mix(h, weight):
        at = h // group * HEAD_SIZE
        v_all = jnp.concatenate(
            [v_ref[:, :, at:at + HEAD_SIZE].reshape(n_seq * keys, HEAD_SIZE), ones_v], axis=1
        )
        mixed = dot(weight, v_all)
        own = pl.ds(h * HEAD_SIZE, HEAD_SIZE)
        out_ref[:, own] = (mixed[:, :HEAD_SIZE] / mixed[:, HEAD_SIZE:]).astype(BF16)
        if outs:
            outs[-1].start()
        outs.append(pltpu.make_async_copy(out_ref.at[:, own], out_hbm.at[0, :, own], out_sem.at[h]))

    for step in range(2 * heads):
        if step in stages:
            stages[step]()
        if step == heads:
            for copy in kv_copies[2 * (n_seq - 1):]:
                copy.wait_recv()
        if step < heads:
            p_ref[step] = weights(step)
        else:
            mix(step - heads, p_ref[step - heads])
    outs[-1].start()

    for copy in pending[n_plane - 1 + n_dp - 1:]:
        copy.wait_recv()
    own_piece.wait()
    for copy in outs:
        copy.wait()
    core_copy.wait_send()
    for copy in kv_copies + pending:
        copy.wait_send()


def write_out(plan, out_hbm, all_hbm, out, gf_out, gd_out, gu_out,
              out_vm, all_vm, gf_vm, gd_vm, gu_vm, load_sem, store_sem):
    rows = out_vm.shape[1] // PIECES
    parts = [(0, pl.ds(piece * rows, rows)) for piece in range(PIECES)]
    gathered = pltpu.make_async_copy(all_hbm, all_vm, load_sem.at[PIECES])
    gathered.start()
    loads = [
        pltpu.make_async_copy(out_hbm.at[at], out_vm.at[at], load_sem.at[i]) for i, at in enumerate(parts)
    ]
    stores = [
        pltpu.make_async_copy(out_vm.at[at], out.at[at], store_sem.at[i]) for i, at in enumerate(parts)
    ]
    for load in loads:
        load.start()
    gathered.wait()
    for index, (which, row, begin, width) in enumerate(plan.halves):
        half = index % 2 * ROWS
        value = all_vm[plan.where(index // 2)].astype(F32)[half:half + ROWS, :width]
        (gf_vm, gd_vm, gu_vm)[which][row:row + ROWS, begin:begin + width] = value
    for load, store in zip(loads, stores):
        load.wait()
        store.start()
    for n, (held, target) in enumerate(((gf_vm, gf_out), (gd_vm, gd_out), (gu_vm, gu_out))):
        stores.append(pltpu.make_async_copy(held, target, store_sem.at[PIECES + n]))
        stores[-1].start()
    for store in stores:
        store.wait()


def on_device(mesh_shape, *args):
    x, sq, cot, w, ad, au, tq, tk, tv, pos = args
    n_grp, n_dp, n_seq = mesh_shape["grp"], mesh_shape["dp"], mesh_shape["seq"]
    plan = Plan(n_grp, n_dp, n_seq, w.shape, x.shape[2], sq.shape[2])
    n_plane, per = plan.plane, plan.per
    rows, queries, keys = sq.shape[1], tq.shape[1], tk.shape[1]
    vm, dma = pltpu.VMEM, pltpu.SemaphoreType.DMA
    unit = (16, LANES)
    shapes = (
        jax.ShapeDtypeStruct(tq.shape, BF16),
        jax.ShapeDtypeStruct((plan.feature_rows, w.shape[1]), F32),
        jax.ShapeDtypeStruct((ad.shape[0], plan.down_width), F32),
        jax.ShapeDtypeStruct((au.shape[0], plan.up_width), F32),
    )
    results = pl.pallas_call(
        functools.partial(kernel, plan),
        out_shape=(shapes[0], jax.ShapeDtypeStruct((2, n_plane, per) + unit, BF16)),
        in_specs=[pl.BlockSpec(memory_space=pl.ANY)] * 10,
        out_specs=[pl.BlockSpec(memory_space=pl.ANY)] * 2,
        scratch_shapes=[
            vm(x.shape[1:], BF16), vm(sq.shape[1:], BF16), vm(cot.shape[1:], BF16), vm(w.shape, BF16),
            vm(ad.shape, BF16), vm(au.shape, BF16), vm(tq.shape[1:], BF16),
            vm((n_seq, keys, tk.shape[2]), BF16), vm((n_seq, keys, tv.shape[2]), BF16),
            vm((n_seq, 1, keys), jnp.int32),
            vm((queries, n_seq * keys), F32), vm((rows, sq.shape[2]), BF16),
            vm(w.shape, F32), vm(ad.shape, F32), vm(au.shape, F32),
            vm((2, n_plane, n_dp, per) + unit, BF16),
            vm((n_plane, n_dp, per) + unit, BF16), vm((n_plane, n_dp, per) + unit, BF16),
            vm((n_plane, n_dp, per) + unit, BF16),
            vm((n_dp, per) + unit, BF16), vm((n_dp, per) + unit, BF16),
            vm((per,) + unit, BF16), vm((tq.shape[2] // HEAD_SIZE, queries, n_seq * keys), BF16),
            dma((10,)), dma((3, n_seq)), dma((3, n_seq)), dma, dma,
            dma((n_plane,)), dma((n_plane,)), dma((n_dp,)), dma((n_dp,)),
            dma((2 * n_plane,)), dma((2 * n_plane,)),
            vm(tq.shape[1:], BF16), dma((tq.shape[2] // HEAD_SIZE,)), dma,
        ],
        compiler_params=pltpu.CompilerParams(
            collective_id=0, has_side_effects=True, vmem_limit_bytes=VMEM_BYTES
        ),
    )(*args)
    return pl.pallas_call(
        functools.partial(write_out, plan),
        out_shape=shapes,
        in_specs=[pl.BlockSpec(memory_space=pl.ANY)] * 2,
        out_specs=[pl.BlockSpec(memory_space=pl.ANY)] * 4,
        scratch_shapes=[vm(tq.shape, BF16), vm((2, n_plane, per) + unit, BF16)]
        + [vm(shape.shape, F32) for shape in shapes[1:]] + [dma((3 + PIECES,))] * 2,
        compiler_params=pltpu.CompilerParams(vmem_limit_bytes=VMEM_BYTES),
    )(*results)


def solution(mesh):
    rows = P(("grp", "dp"), "seq", None)
    return jax.shard_map(
        functools.partial(on_device, dict(mesh.shape)),
        mesh=mesh,
        in_specs=(rows, rows, rows, P(), P(), P(), rows, rows, rows, P(("grp", "dp"), "seq")),
        out_specs=(rows, P("dp", None), P(None, "dp"), P(None, "dp")),
        check_vma=False,
    )
```
